16 devices in a mesh: data: 4 (over z, y), model: 4 (over x, core).
Axes of the slice: x: 2, y: 2, z: 2, core: 2. Of those that a mesh axis runs over, the one named last changes fastest.
Arguments:
- hidden: bfloat16 [8192, 6144], P('data', 'model')
- unembed: bfloat16 [50432, 6144], P('model', 'data')
- draft_ids: int32 [8192], P('data')
- q_prob: float32 [8192], P('data')
Outputs:
- output 1: float32 [8192], P('data')
- output 2: float32 [8192], P('data')
All inputs are finite; a program needn't handle non-finite values.
Results may differ from the reference program's by a relative error of at most 0.001.
Values are sent between devices in bfloat16 or wider.
A program may use at most 1 GiB of HBM per device.

```python
import math
import jax
import jax.numpy as jnp
from jax import lax

VOCAB = 50432
WIDTH = 6144
ROWS = 8192
ROW_BLOCK = 64


def setup_inputs(seed: int = 0) -> dict:
    base_key = jax.random.key(seed)
    k_hid, k_wt, k_draft, k_prob = jax.random.split(base_key, 4)
    hidden = jax.random.normal(k_hid, (ROWS, WIDTH), jnp.float32).astype(jnp.bfloat16)
    unembed = (jax.random.normal(k_wt, (VOCAB, WIDTH), jnp.float32) * WIDTH ** -0.5).astype(jnp.bfloat16)
    draft_ids = jax.random.randint(k_draft, (ROWS,), 0, VOCAB, jnp.int32).at[0].set(VOCAB - 1)
    log_q = -math.log(VOCAB) - 0.5 + jax.random.uniform(k_prob, (ROWS,), jnp.float32, -1.0, 1.0)
    q_prob = jnp.exp(log_q)
    return {"hidden": hidden, "unembed": unembed, "draft_ids": draft_ids, "q_prob": q_prob}


def reference(hidden, unembed, draft_ids, q_prob):
    blocks = ROWS // ROW_BLOCK
    vocab_ids = jnp.arange(VOCAB, dtype=jnp.int32)[None, :]

    def one_block(block_in):
        h_blk, d_blk = block_in
        logits = jnp.dot(h_blk, unembed.T, preferred_element_type=jnp.float32)
        row_max = jnp.max(logits, axis=1)
        log_sum = row_max + jnp.log(jnp.sum(jnp.exp(logits - row_max[:, None]), axis=1))
        picked = jnp.sum(jnp.where(vocab_ids == d_blk[:, None], logits, 0.0), axis=1)
        return picked - log_sum

    log_prob = lax.map(one_block, (hidden.reshape(blocks, ROW_BLOCK, WIDTH), draft_ids.reshape(blocks, ROW_BLOCK))).reshape(ROWS)
    accept = jnp.minimum(1.0, jnp.exp(log_prob) / q_prob)
    return log_prob, accept
```

```python
import functools

import jax
import jax.numpy as jnp
from jax import lax
from jax.experimental import pallas as pl
from jax.experimental.pallas import tpu as pltpu
from jax.sharding import PartitionSpec as P

MESH = pl.DeviceIdType.MESH
SUBS = 4
TILES = 16
X_STEP = 34.0
W_TIMES = (87.0, 174.0, 261.0, 382.0, 469.0, 522.0, 575.0, 620.0)


def tile_of(q):
    if q < 4:
        return 0, q
    if q < 12:
        return 1 + q % 2, (q - 4) // 2
    return 3, q - 12


def plan(n_chunks):
    items = []
    w_times = [W_TIMES[-1] * (j + 1) / n_chunks for j in range(n_chunks)] if n_chunks != len(W_TIMES) else W_TIMES
    for q in range(TILES):
        items.append((X_STEP * (q + 1), 0, ("x", q)))
        items.append((X_STEP * (q + 1) + 4.0, 2, ("h", q)))
    for i, t in enumerate((34.0, 121.0, 208.0, 329.0)):
        items.append((t, 1, ("yz", i)))
    for i, t in enumerate((330.0, 331.0, 416.0, 417.0)):
        items.append((t, 1, ("diag", i)))
    for j in range(n_chunks):
        items.append((w_times[j], 3, ("w", j)))
    items.sort()
    runs, events, n_h, n_w = [], [], 0, 0
    for _, _, (kind, k) in items:
        events.append((kind, k))
        if kind == "h":
            if n_w:
                runs.append((events, (k, 0, 0, 1, n_w)))
                events = []
            n_h += 1
        if kind == "w":
            if n_h:
                runs.append((events, (0, 1, k, 0, n_h)))
                events = []
            n_w += 1
    assert not events
    return runs


def kernel(
    v_tile, h_ref, w_ref, ids_ref, q_ref, lp_ref, acc_ref, hbuf,
    wv, hv, ids_all, mx, sm, pk, st_send, st_recv,
    ss, rs, wss, wrs, wls, iss, irs, ils, sss, srs, lsem,
):
    rows, kp = h_ref.shape
    tile = rows // SUBS
    vocab = w_ref.shape[0]
    share = vocab // 4
    n_chunks = -(-share // v_tile)
    runs = plan(n_chunks)

    d, m = lax.axis_index("data"), lax.axis_index("model")
    y, z = lax.rem(d, 2), d // 2
    core, x = lax.rem(m, 2), m // 2
    m_sib = m + 1 - 2 * core
    m_x = m + 2 - 4 * x
    m_xs = m_sib + 2 - 4 * x

    def block(rb):
        ry, rz = rb % 2, rb // 2
        yy = 1 - y if ry else y
        zz = 1 - z if rz else z
        return zz * 2 + yy

    def row0(q):
        rb, sub = tile_of(q)
        return pl.multiple_of(block(rb) * rows + sub * tile, tile)

    def own_piece(q):
        rb, sub = tile_of(q)
        return h_ref.at[pl.ds(sub * tile, tile), :] if rb == 0 else hbuf.at[m, pl.ds(row0(q), tile), :]

    def send_h(src, q_here, q_there, mm, dev, sem):
        return pltpu.make_async_remote_copy(
            src_ref=src, dst_ref=hbuf.at[mm, pl.ds(row0(q_here), tile), :], send_sem=ss.at[sem],
            recv_sem=rs.at[q_there * 4 + mm], device_id=dev, device_id_type=MESH)

    def wait_h(q, mm):
        pltpu.make_async_remote_copy(
            src_ref=hbuf.at[mm, pl.ds(row0(q), tile), :], dst_ref=hbuf.at[mm, pl.ds(row0(q), tile), :],
            send_sem=ss.at[0], recv_sem=rs.at[q * 4 + mm], device_id=(d, m), device_id_type=MESH).wait_recv()

    def w_size(j):
        return min(v_tile, share - j * v_tile)

    def send_w(j, rb):
        size, dd = w_size(j), block(rb)
        return pltpu.make_async_remote_copy(
            src_ref=w_ref.at[pl.ds(pl.multiple_of(dd * share + j * v_tile, 8), size), :],
            dst_ref=wv.at[pl.ds(j * v_tile, size), pl.ds(pl.multiple_of(d * kp, kp), kp)],
            send_sem=wss.at[j * 4 + rb], recv_sem=wrs.at[j * 4 + rb], device_id=(dd, m), device_id_type=MESH)

    def wait_w(j, rb):
        size, dd = w_size(j), block(rb)
        pltpu.make_async_remote_copy(
            src_ref=w_ref.at[pl.ds(0, size), :],
            dst_ref=wv.at[pl.ds(j * v_tile, size), pl.ds(pl.multiple_of(dd * kp, kp), kp)],
            send_sem=wss.at[j * 4 + rb], recv_sem=wrs.at[j * 4 + rb], device_id=(d, m), device_id_type=MESH).wait_recv()

    def local_w(j):
        size = w_size(j)
        return pltpu.make_async_copy(
            w_ref.at[pl.ds(pl.multiple_of(d * share + j * v_tile, 8), size), :],
            wv.at[pl.ds(j * v_tile, size), pl.ds(pl.multiple_of(d * kp, kp), kp)], wls.at[j])

    def send_ids(rb):
        return pltpu.make_async_remote_copy(
            src_ref=ids_ref, dst_ref=ids_all.at[rb], send_sem=iss.at[rb], recv_sem=irs.at[rb],
            device_id=(block(rb), m), device_id_type=MESH)

    def over_y(i):
        send_h(own_piece(i), i, 4 + 2 * i, m, (block(1), m), 48 + i).start()

    def over_z(i):
        send_h(own_piece(i), i, 5 + 2 * i, m, (block(2), m), 52 + i).start()

    def weights(j):
        if j < n_chunks:
            for rb in (3, 1, 2):
                send_w(j, rb).start()

    def spread(q):
        send_h(own_piece(q), q, q, m, (d, m_x), q).start()
        send_h(own_piece(q), q, q, m, (d, m_sib), 16 + q).start()

    def event(kind, k):
        if kind == "x":
            wait_h(k, m_x)
            send_h(hbuf.at[m_x, pl.ds(row0(k), tile), :], k, k, m_x, (d, m_sib), 32 + k).start()
        elif kind == "h":
            wait_h(k, m_sib)
            wait_h(k, m_xs)
        elif kind == "yz":
            wait_h(4 + 2 * k, m)
            wait_h(5 + 2 * k, m)
            if k % 2 == 0:
                send_h(own_piece(5 + 2 * k), 5 + 2 * k, 12 + k, m, (block(1), m), 56 + k).start()
            else:
                send_h(own_piece(4 + 2 * k), 4 + 2 * k, 12 + k, m, (block(2), m), 56 + k).start()
            spread(4 + 2 * k)
            spread(5 + 2 * k)
            if k == 1:
                over_y(3)
                over_z(3)
                weights(3)
            elif k == 2:
                weights(4)
            elif k == 3:
                for j in range(5, n_chunks):
                    weights(j)
        elif kind == "diag":
            wait_h(12 + k, m)
            spread(12 + k)
        else:
            local_w(k).wait()
            for rb in (1, 2, 3):
                wait_w(k, rb)

    def rb_sub(q):
        mid = q >= 4
        late = q >= 12
        rb = jnp.where(late, 3, jnp.where(mid, 1 + lax.rem(q, 2), 0))
        sub = jnp.where(late, q - 12, jnp.where(mid, (q - 4) // 2, q))
        return rb, sub

    def load_parts(q, slot, act):
        rb, sub = rb_sub(q)
        ry, rz = lax.rem(rb, 2), rb // 2
        yy, zz = y + ry - 2 * y * ry, z + rz - 2 * z * rz
        row = pl.multiple_of((zz * 2 + yy) * rows + sub * tile, tile)
        for mm in range(4):
            dst = hv.at[slot, :, pl.ds(mm * kp, kp)]
            mine = jnp.logical_and(rb == 0, m == mm)

            @pl.when(mine)
            def _():
                act(pltpu.make_async_copy(h_ref.at[pl.ds(pl.multiple_of(sub * tile, tile), tile), :], dst, lsem.at[slot * 4 + mm]))

            @pl.when(jnp.logical_not(mine))
            def _():
                act(pltpu.make_async_copy(hbuf.at[mm, pl.ds(row, tile), :], dst, lsem.at[slot * 4 + mm]))

    def wait_parts(slot):
        for mm in range(4):
            pltpu.make_async_copy(
                h_ref.at[pl.ds(0, tile), :], hv.at[slot, :, pl.ds(mm * kp, kp)], lsem.at[slot * 4 + mm]).wait()

    own_ids = pltpu.make_async_copy(ids_ref, ids_all.at[0], ils)
    own_ids.start()
    for rb in (1, 2, 3):
        send_ids(rb).start()
    for i in range(3):
        over_y(i)
        over_z(i)
        if i == 0:
            for q in range(4):
                spread(q)
        weights(i)
    for j in range(n_chunks):
        local_w(j).start()
    mx[...] = jnp.full(mx.shape, -jnp.inf, jnp.float32)
    sm[...] = jnp.zeros(sm.shape, jnp.float32)
    pk[...] = jnp.zeros(pk.shape, jnp.float32)
    own_ids.wait()
    for rb in (1, 2, 3):
        send_ids(rb).wait()

    first_events, first_run = runs[0]
    for e in first_events:
        event(*e)
    load_parts(jnp.int32(first_run[0]), 0, lambda c: c.start())

    base = m * vocab + d * share

    def compute(q, j, slot):
        start = pl.multiple_of(jnp.minimum(j * v_tile, share - v_tile), 8)
        skip = j * v_tile - start
        logits = lax.dot_general(
            wv[pl.ds(start, v_tile), :], hv[slot], (((1,), (1,)), ((), ())), preferred_element_type=jnp.float32)
        local = lax.broadcasted_iota(jnp.int32, (v_tile, tile), 0)
        fresh = local >= skip
        rb, sub = rb_sub(q)
        want = ids_all[rb, sub] - (base + start)
        logits = jnp.where(fresh, logits, -jnp.inf)
        hit = jnp.logical_and(fresh, local == want)
        old = mx[q]
        stack = logits.reshape(v_tile // 8, 8, tile)
        new = jnp.maximum(old, jnp.max(stack, axis=0))
        grown = jnp.sum(jnp.exp(stack - new[None]), axis=0)
        sm[q] = sm[q] * jnp.exp(old - new) + grown
        mx[q] = new
        pk[q] = pk[q] + jnp.sum(jnp.where(hit, logits, 0.0).reshape(v_tile // 8, 8, tile), axis=0)

    n_runs = len(runs)

    def pick(r, values):
        out = jnp.int32(values[0])
        for i in range(1, len(values)):
            if values[i] != values[i - 1]:
                out = jnp.where(r >= i, jnp.int32(values[i]), out)
        return out

    q0s, dqs, j0s, djs, ns = (tuple(run[i] for _, run in runs) for i in range(5))

    def run_body(r, s0):
        q0, dq, j0, dj, n = (pick(r, v) for v in (q0s, dqs, j0s, djs, ns))
        q_next = pick(r, q0s[1:] + (0,))

        def step(i, carry):
            s = s0 + i
            slot = lax.rem(s, 2)
            last = i == n - 1

            @pl.when(last)
            def _():
                for k in range(1, n_runs):
                    if runs[k][0]:
                        @pl.when(r == k - 1)
                        def _(k=k):
                            for e in runs[k][0]:
                                event(*e)

            @pl.when(jnp.logical_not(jnp.logical_and(last, r == n_runs - 1)))
            def _():
                load_parts(jnp.where(last, q_next, q0 + dq * (i + 1)), 1 - slot, lambda c: c.start())

            wait_parts(slot)
            compute(q0 + dq * i, j0 + dj * i, slot)
            return carry

        lax.fori_loop(0, n, step, 0)
        return s0 + n

    lax.fori_loop(0, n_runs, run_body, jnp.int32(0))

    lanes = 128
    for q in range(TILES):
        rb, sub = tile_of(q)
        old = mx[q]
        top = jnp.max(old, axis=0, keepdims=True)
        parts = (top, jnp.sum(sm[q] * jnp.exp(old - top), axis=0, keepdims=True), jnp.sum(pk[q], axis=0, keepdims=True))
        for k, part in enumerate(parts):
            for i in range(tile // lanes):
                st_send[rb, k, pl.ds(sub * (tile // lanes) + i, 1), :] = part[:, i * lanes:(i + 1) * lanes]

    me = d * 4 + m
    st_recv[me] = st_send[0]

    def send_stats(rb, o):
        return pltpu.make_async_remote_copy(
            src_ref=st_send.at[rb], dst_ref=st_recv.at[me], send_sem=sss.at[rb * 4 + o], recv_sem=srs.at[me],
            device_id=(block(rb), lax.rem(m + o, 4)), device_id_type=MESH)

    others = [(rb, o) for rb in (3, 2, 1, 0) for o in range(4) if (rb, o) != (0, 0)]
    for rb, o in others:
        send_stats(rb, o).start()

    def drain(i, carry):
        pltpu.make_async_remote_copy(
            src_ref=h_ref.at[pl.ds(0, tile), :], dst_ref=hbuf.at[0, pl.ds(0, tile), :], send_sem=ss.at[i],
            recv_sem=rs.at[0], device_id=(d, m), device_id_type=MESH).wait_send()
        return carry

    lax.fori_loop(0, 60, drain, 0)
    for j in range(n_chunks):
        for rb in (1, 2, 3):
            send_w(j, rb).wait_send()
    for rb, o in others:
        send_stats(rb, o).wait_send()
    for rb, o in others:
        source = block(rb) * 4 + lax.rem(m + o, 4)
        pltpu.make_async_remote_copy(
            src_ref=st_send.at[rb], dst_ref=st_recv.at[source], send_sem=sss.at[rb * 4 + o], recv_sem=srs.at[source],
            device_id=(d, m), device_id_type=MESH).wait_recv()

    top = jnp.max(st_recv[:, 0], axis=0)
    total = jnp.sum(st_recv[:, 1] * jnp.exp(st_recv[:, 0] - top[None]), axis=0)
    picked = jnp.sum(st_recv[:, 2], axis=0)
    log_prob = picked - (top + jnp.log(total))
    lp_ref[...] = log_prob
    acc_ref[...] = jnp.minimum(1.0, jnp.exp(log_prob) / q_ref[...])


def build(mesh, v_tile):
    def per_device(h_part, w_part, draft_loc, q_loc):
        rows, kp = h_part.shape
        vocab = w_part.shape[0]
        share, tile = vocab // 4, rows // SUBS
        n_chunks = -(-share // v_tile)
        lanes = 128
        flat = (rows // lanes, lanes)
        dma, vmem = pltpu.SemaphoreType.DMA, pltpu.VMEM
        any_space = pl.BlockSpec(memory_space=pl.ANY)
        in_vmem = pl.BlockSpec(memory_space=pltpu.VMEM)
        lp, acc, _ = pl.pallas_call(
            functools.partial(kernel, v_tile),
            out_shape=(
                jax.ShapeDtypeStruct(flat, jnp.float32),
                jax.ShapeDtypeStruct(flat, jnp.float32),
                jax.ShapeDtypeStruct((4, 4 * rows, kp), jnp.bfloat16),
            ),
            in_specs=[any_space, any_space, in_vmem, in_vmem],
            out_specs=(in_vmem, in_vmem, any_space),
            scratch_shapes=[
                vmem((share, 4 * kp), jnp.bfloat16),
                vmem((2, tile, 4 * kp), jnp.bfloat16),
                vmem((4, SUBS, 1, tile), jnp.int32),
                vmem((TILES, 8, tile), jnp.float32),
                vmem((TILES, 8, tile), jnp.float32),
                vmem((TILES, 8, tile), jnp.float32),
                vmem((4, 3) + flat, jnp.float32),
                vmem((16, 3) + flat, jnp.float32),
                dma((60,)), dma((64,)), dma((4 * n_chunks,)), dma((4 * n_chunks,)), dma((n_chunks,)),
                dma((4,)), dma((4,)), dma, dma((16,)), dma((16,)), dma((8,)),
            ],
            compiler_params=pltpu.CompilerParams(has_side_effects=True, vmem_limit_bytes=66_000_000),
            name="head",
        )(h_part, w_part, draft_loc.reshape(SUBS, 1, tile), q_loc.reshape(flat))
        return lp.reshape(rows), acc.reshape(rows)

    return jax.shard_map(
        per_device, mesh=mesh, in_specs=(P("data", "model"), P("model", "data"), P("data"), P("data")),
        out_specs=(P("data"), P("data")), check_vma=False)


def solution(mesh):
    return build(mesh, 400)
```

```python
import functools

import jax
import jax.numpy as jnp
from jax import lax
from jax.experimental import pallas as pl
from jax.experimental.pallas import tpu as pltpu
from jax.sharding import PartitionSpec as P

MESH = pl.DeviceIdType.MESH
SUBS = 4
TILES = 16
FLOOR = float(jnp.finfo(jnp.float32).min)
LINK_ORDER = ("H0", "H1", "W0", "W1", "W2", "F0", "F1", "H2", "H3", "W3", "W4", "F2", "F3", "W5", "W6", "W7")
H_TIME, W_TIME, STEP_TIME, LAG = 33.7, 414.0, 2.8, 3.0
MAX_RUN = 3


def tile_of(q):
    if q < 4:
        return 0, q
    if q < 12:
        return 1 + q % 2, (q - 4) // 2
    return 3, q - 12


def link_order(n_chunks):
    tokens = [(t[0], int(t[1:])) for t in LINK_ORDER]
    last = max(k for kind, k in tokens if kind == "W")
    tokens = [t for t in tokens if t[0] != "W" or t[1] < n_chunks] + [("W", j) for j in range(last + 1, n_chunks)]
    start, after = [], [[], [], [], []]
    current = start
    for kind, k in tokens:
        if kind == "F":
            current = after[k // 2 * 2 + 1]
        current.append((kind, k))
    return start, after


def stretches(values):
    out, i = [], 0
    while i < len(values):
        n = 1
        while n < MAX_RUN and i + n < len(values) and values[i + n] == values[i] + n:
            n += 1
        out.append((n, values[i]))
        i += n
    return out


def plan(sizes):
    start, after = link_order(len(sizes))
    free, done, at = {"x": 0.0, "y": 0.0, "z": 0.0}, {}, {}
    tiles, chunks, cells, runs, pending = [], [], set(), [], []
    n_main = len(sizes) - 1

    def put(link, token, now):
        free[link] = max(free[link], now) + (W_TIME * sizes[token[1]] / sum(sizes) if token[0] == "W" else H_TIME)
        done[link, token] = free[link]

    def put_x(q, now):
        put("x", ("X", q), now)
        at["x", q] = free["x"] + LAG

    def issue(token, now):
        kind, k = token
        for link in "yz" if kind != "F" else "yz"[k % 2]:
            put(link, token, now)
        if kind == "F":
            at["diag", k] = done["yz"[k % 2], token] + LAG
        else:
            at["yz" if kind == "H" else "w", k] = max(done["y", token], done["z", token]) + LAG

    def handle(e, now):
        kind, k = e
        del at[e]
        pending.append(e)
        if kind == "x":
            at["h", k] = now + LAG
        elif kind == "h":
            tiles.append(k)
        elif kind == "yz":
            put_x(4 + 2 * k, now)
            put_x(5 + 2 * k, now)
            for token in after[k]:
                issue(token, now)
        elif kind == "diag":
            put_x(12 + k, now)
        elif k < n_main:
            chunks.append(k)

    def first():
        return min(at, key=lambda e: (at[e], e))

    for token in start:
        issue(token, 0.0)
    for q in range(4):
        put_x(q, 0.0)
    now = 0.0
    while len(cells) < TILES * n_main:
        while at and at[first()] <= now:
            handle(first(), now)
        options = [
            (n, (q, 0, j, 1, n)) for q in sorted(tiles)
            for n, j in stretches([j for j in sorted(chunks) if (q, j) not in cells])]
        options += [
            (n, (q, 1, j, 0, n)) for j in sorted(chunks)
            for n, q in stretches([q for q in sorted(tiles) if (q, j) not in cells])]
        if not options:
            e = first()
            now = max(now, at[e])
            handle(e, now)
            continue
        _, run = max(options, key=lambda o: o[0])
        q, dq, j, dj, n = run
        cells.update((q + dq * i, j + dj * i) for i in range(n))
        now += (n if runs else n - 1) * STEP_TIME
        runs.append((pending[:], run))
        pending.clear()
    while at:
        handle(first(), now)
    return runs, pending


def kernel(
    v_tile, h_ref, w_ref, ids_ref, q_ref, lp_ref, acc_ref, hbuf,
    wv, hv, lg, lg_end, ids_all, mx, sm, pk, st_send, st_recv,
    ss, rs, wss, wrs, wls, iss, irs, ils, sss, srs, lsem,
):
    rows, kp = h_ref.shape
    tile = rows // SUBS
    vocab = w_ref.shape[0]
    share = vocab // 4
    n_chunks = -(-share // v_tile)
    sizes = [min(v_tile, share - j * v_tile) for j in range(n_chunks)]
    runs, leftover = plan(sizes)
    send_first, send_after = link_order(n_chunks)

    d, m = lax.axis_index("data"), lax.axis_index("model")
    y, z = lax.rem(d, 2), d // 2
    core, x = lax.rem(m, 2), m // 2
    m_sib = m + 1 - 2 * core
    m_x = m + 2 - 4 * x
    m_xs = m_sib + 2 - 4 * x

    def block(rb):
        ry, rz = rb % 2, rb // 2
        yy = 1 - y if ry else y
        zz = 1 - z if rz else z
        return zz * 2 + yy

    def row0(q):
        rb, sub = tile_of(q)
        return pl.multiple_of(block(rb) * rows + sub * tile, tile)

    def own_piece(q):
        rb, sub = tile_of(q)
        return h_ref.at[pl.ds(sub * tile, tile), :] if rb == 0 else hbuf.at[m, pl.ds(row0(q), tile), :]

    def send_h(src, q_here, q_there, mm, dev, sem):
        return pltpu.make_async_remote_copy(
            src_ref=src, dst_ref=hbuf.at[mm, pl.ds(row0(q_here), tile), :], send_sem=ss.at[sem],
            recv_sem=rs.at[q_there * 4 + mm], device_id=dev, device_id_type=MESH)

    def wait_h(q, mm):
        pltpu.make_async_remote_copy(
            src_ref=hbuf.at[mm, pl.ds(row0(q), tile), :], dst_ref=hbuf.at[mm, pl.ds(row0(q), tile), :],
            send_sem=ss.at[0], recv_sem=rs.at[q * 4 + mm], device_id=(d, m), device_id_type=MESH).wait_recv()

    def send_w(j, rb):
        size, dd = sizes[j], block(rb)
        return pltpu.make_async_remote_copy(
            src_ref=w_ref.at[pl.ds(pl.multiple_of(dd * share + j * v_tile, 8), size), :],
            dst_ref=wv.at[pl.ds(j * v_tile, size), pl.ds(pl.multiple_of(d * kp, kp), kp)],
            send_sem=wss.at[j * 4 + rb], recv_sem=wrs.at[j * 4 + rb], device_id=(dd, m), device_id_type=MESH)

    def wait_w(j, rb):
        size, dd = sizes[j], block(rb)
        pltpu.make_async_remote_copy(
            src_ref=w_ref.at[pl.ds(0, size), :],
            dst_ref=wv.at[pl.ds(j * v_tile, size), pl.ds(pl.multiple_of(dd * kp, kp), kp)],
            send_sem=wss.at[j * 4 + rb], recv_sem=wrs.at[j * 4 + rb], device_id=(d, m), device_id_type=MESH).wait_recv()

    def local_w(j):
        size = sizes[j]
        return pltpu.make_async_copy(
            w_ref.at[pl.ds(pl.multiple_of(d * share + j * v_tile, 8), size), :],
            wv.at[pl.ds(j * v_tile, size), pl.ds(pl.multiple_of(d * kp, kp), kp)], wls.at[j])

    def send_ids(rb):
        return pltpu.make_async_remote_copy(
            src_ref=ids_ref, dst_ref=ids_all.at[rb], send_sem=iss.at[rb], recv_sem=irs.at[rb],
            device_id=(block(rb), m), device_id_type=MESH)

    def put(kind, k):
        if kind == "H":
            send_h(own_piece(k), k, 4 + 2 * k, m, (block(1), m), 48 + k).start()
            send_h(own_piece(k), k, 5 + 2 * k, m, (block(2), m), 52 + k).start()
        elif kind == "F":
            q = 5 + 2 * k if k % 2 == 0 else 4 + 2 * k
            send_h(own_piece(q), q, 12 + k, m, (block(1 + k % 2), m), 56 + k).start()
        else:
            for rb in (3, 1, 2):
                send_w(k, rb).start()

    def spread(q):
        send_h(own_piece(q), q, q, m, (d, m_x), q).start()
        send_h(own_piece(q), q, q, m, (d, m_sib), 16 + q).start()

    def event(kind, k):
        if kind == "x":
            wait_h(k, m_x)
            send_h(hbuf.at[m_x, pl.ds(row0(k), tile), :], k, k, m_x, (d, m_sib), 32 + k).start()
        elif kind == "h":
            wait_h(k, m_sib)
            wait_h(k, m_xs)
        elif kind == "yz":
            wait_h(4 + 2 * k, m)
            wait_h(5 + 2 * k, m)
            spread(4 + 2 * k)
            spread(5 + 2 * k)
            for token in send_after[k]:
                put(*token)
        elif kind == "diag":
            wait_h(12 + k, m)
            spread(12 + k)
        else:
            local_w(k).wait()
            for rb in (1, 2, 3):
                wait_w(k, rb)

    def rb_sub(q):
        mid = q >= 4
        late = q >= 12
        rb = jnp.where(late, 3, jnp.where(mid, 1 + lax.rem(q, 2), 0))
        sub = jnp.where(late, q - 12, jnp.where(mid, (q - 4) // 2, q))
        return rb, sub

    def load_parts(q, slot):
        rb, sub = rb_sub(q)
        ry, rz = lax.rem(rb, 2), rb // 2
        yy, zz = y + ry - 2 * y * ry, z + rz - 2 * z * rz
        row = pl.multiple_of((zz * 2 + yy) * rows + sub * tile, tile)

        def part(mm, own):
            src = h_ref.at[pl.ds(pl.multiple_of(sub * tile, tile), tile), :] if own else hbuf.at[mm, pl.ds(row, tile), :]
            pltpu.make_async_copy(src, hv.at[slot, :, pl.ds(mm * kp, kp)], lsem.at[slot * 4 + mm]).start()

        @pl.when(rb != 0)
        def _():
            for mm in range(4):
                part(mm, False)

        @pl.when(rb == 0)
        def _():
            for mm in range(4):
                pl.when(m == mm)(functools.partial(part, mm, True))
                pl.when(m != mm)(functools.partial(part, mm, False))

    def wait_parts(slot):
        for mm in range(4):
            pltpu.make_async_copy(
                h_ref.at[pl.ds(0, tile), :], hv.at[slot, :, pl.ds(mm * kp, kp)], lsem.at[slot * 4 + mm]).wait()

    own_ids = pltpu.make_async_copy(ids_ref, ids_all.at[0], ils)
    own_ids.start()
    for rb in (1, 2, 3):
        send_ids(rb).start()
    for i, token in enumerate(send_first):
        put(*token)
        if i == 0:
            for q in range(4):
                spread(q)
    for j in range(n_chunks):
        local_w(j).start()
    mx[...] = jnp.full(mx.shape, FLOOR, jnp.float32)
    sm[...] = jnp.zeros(sm.shape, jnp.float32)
    pk[...] = jnp.zeros(pk.shape, jnp.float32)
    lg[...] = jnp.full(lg.shape, -jnp.inf, jnp.float32)
    lg_end[...] = jnp.full(lg_end.shape, -jnp.inf, jnp.float32)
    own_ids.wait()
    for rb in (1, 2, 3):
        send_ids(rb).wait()

    base = m * vocab + d * share
    nowhere = jnp.int32(1 << 30)

    def product(start, size, slot):
        return lax.dot_general(
            wv[pl.ds(start, size), :], hv[slot], (((1,), (1,)), ((), ())), preferred_element_type=jnp.float32)

    def absorb(ref, q, start):
        rb, sub = rb_sub(q)
        size = ref.shape[0]
        spot = ids_all[rb, sub] - (base + start) - lax.broadcasted_iota(jnp.int32, (8, tile), 0)
        old = mx[q]
        new = old
        for k in range(0, size, 8):
            new = jnp.maximum(new, ref[k:k + 8, :])
        grown, picked = sm[q] * jnp.exp(old - new), pk[q]
        for k in range(0, size, 8):
            part = ref[k:k + 8, :]
            grown = grown + jnp.exp(part - new)
            picked = picked + jnp.where(spot == k, part, 0.0)
        mx[q] = new
        sm[q] = grown
        pk[q] = picked

    n_runs = len(runs)
    codes = []
    for i, (_, (q0, dq, j0, dj, n)) in enumerate(runs):
        q_next = runs[i + 1][1][0] if i + 1 < n_runs else 0
        codes.append(((((q0 * 2 + dq) * 8 + j0) * 2 + dj) * 8 + n) * 16 + q_next)

    for e in runs[0][0]:
        event(*e)
    load_parts(jnp.int32(runs[0][1][0]), 0)

    def run_body(r, carry):
        code = jnp.int32(codes[0])
        for i in range(1, n_runs):
            code = jnp.where(r >= i, jnp.int32(codes[i]), code)
        q_next, code = lax.rem(code, 16), code // 16
        n, code = lax.rem(code, 8), code // 8
        dj, code = lax.rem(code, 2), code // 2
        j0, code = lax.rem(code, 8), code // 8
        dq, q0 = lax.rem(code, 2), code // 2

        def step(i, carry):
            slot, fresh, q_old, start_old = carry
            q = q0 + dq * i
            last = i == n - 1

            @pl.when(last)
            def _():
                for k in range(1, n_runs):
                    if runs[k][0]:
                        @pl.when(r == k - 1)
                        def _(k=k):
                            for e in runs[k][0]:
                                event(*e)

            q_new = jnp.where(last, q_next, q + dq)
            pl.when(q_new != q)(lambda: load_parts(q_new, 1 - slot))
            pl.when(fresh == 1)(lambda: wait_parts(slot))
            start = pl.multiple_of((j0 + dj * i) * v_tile, 8)
            absorb(lg, q_old, start_old)
            lg[...] = product(start, v_tile, slot)
            return jnp.where(q_new != q, 1 - slot, slot), jnp.where(q_new != q, 1, 0), q, start

        return lax.fori_loop(0, n, step, carry)

    zero = jnp.int32(0)
    slot, fresh, q_old, start_old = lax.fori_loop(0, n_runs, run_body, (zero, jnp.int32(1), zero, nowhere))

    absorb(lg, q_old, start_old)
    for e in leftover:
        event(*e)
    end_start = (n_chunks - 1) * v_tile

    def end_step(q, carry):
        slot, fresh, q_old, start_old = carry
        pl.when(q < TILES - 1)(lambda: load_parts(q + 1, 1 - slot))
        pl.when(fresh == 1)(lambda: wait_parts(slot))
        absorb(lg_end, q_old, start_old)
        lg_end[...] = product(end_start, sizes[-1], slot)
        return 1 - slot, jnp.int32(1), q, jnp.int32(end_start)

    _, _, q_old, start_old = lax.fori_loop(0, TILES, end_step, (slot, fresh, zero, nowhere))
    absorb(lg_end, q_old, start_old)

    lanes = 128
    for q in range(TILES):
        rb, sub = tile_of(q)
        old = mx[q]
        top = jnp.max(old, axis=0, keepdims=True)
        parts = (top, jnp.sum(sm[q] * jnp.exp(old - top), axis=0, keepdims=True), jnp.sum(pk[q], axis=0, keepdims=True))
        for k, part in enumerate(parts):
            for i in range(tile // lanes):
                st_send[rb, k, pl.ds(sub * (tile // lanes) + i, 1), :] = part[:, i * lanes:(i + 1) * lanes]

    me = d * 4 + m
    st_recv[me] = st_send[0]

    def send_stats(rb, o):
        return pltpu.make_async_remote_copy(
            src_ref=st_send.at[rb], dst_ref=st_recv.at[me], send_sem=sss.at[rb * 4 + o], recv_sem=srs.at[me],
            device_id=(block(rb), lax.rem(m + o, 4)), device_id_type=MESH)

    others = [(rb, o) for rb in (3, 2, 1, 0) for o in range(4) if (rb, o) != (0, 0)]
    for rb, o in others:
        send_stats(rb, o).start()

    def drain(i, carry):
        pltpu.make_async_remote_copy(
            src_ref=h_ref.at[pl.ds(0, tile), :], dst_ref=hbuf.at[0, pl.ds(0, tile), :], send_sem=ss.at[i],
            recv_sem=rs.at[0], device_id=(d, m), device_id_type=MESH).wait_send()
        return carry

    lax.fori_loop(0, 60, drain, 0)
    for j in range(n_chunks):
        for rb in (1, 2, 3):
            send_w(j, rb).wait_send()
    for rb, o in others:
        send_stats(rb, o).wait_send()
    for rb, o in others:
        source = block(rb) * 4 + lax.rem(m + o, 4)
        pltpu.make_async_remote_copy(
            src_ref=st_send.at[rb], dst_ref=st_recv.at[source], send_sem=sss.at[rb * 4 + o], recv_sem=srs.at[source],
            device_id=(d, m), device_id_type=MESH).wait_recv()

    top = jnp.max(st_recv[:, 0], axis=0)
    total = jnp.sum(st_recv[:, 1] * jnp.exp(st_recv[:, 0] - top[None]), axis=0)
    picked = jnp.sum(st_recv[:, 2], axis=0)
    log_prob = picked - (top + jnp.log(total))
    lp_ref[...] = log_prob
    acc_ref[...] = jnp.minimum(1.0, jnp.exp(log_prob) / q_ref[...])


def build(mesh, v_tile):
    def per_device(h_part, w_part, draft_loc, q_loc):
        rows, kp = h_part.shape
        vocab = w_part.shape[0]
        share, tile = vocab // 4, rows // SUBS
        n_chunks = -(-share // v_tile)
        lanes = 128
        flat = (rows // lanes, lanes)
        dma, vmem = pltpu.SemaphoreType.DMA, pltpu.VMEM
        any_space = pl.BlockSpec(memory_space=pl.ANY)
        in_vmem = pl.BlockSpec(memory_space=pltpu.VMEM)
        lp, acc, _ = pl.pallas_call(
            functools.partial(kernel, v_tile),
            out_shape=(
                jax.ShapeDtypeStruct(flat, jnp.float32),
                jax.ShapeDtypeStruct(flat, jnp.float32),
                jax.ShapeDtypeStruct((4, 4 * rows, kp), jnp.bfloat16),
            ),
            in_specs=[any_space, any_space, in_vmem, in_vmem],
            out_specs=(in_vmem, in_vmem, any_space),
            scratch_shapes=[
                vmem((share, 4 * kp), jnp.bfloat16),
                vmem((2, tile, 4 * kp), jnp.bfloat16),
                vmem((v_tile, tile), jnp.float32),
                vmem((share - (n_chunks - 1) * v_tile, tile), jnp.float32),
                vmem((4, SUBS, 1, tile), jnp.int32),
                vmem((TILES, 8, tile), jnp.float32),
                vmem((TILES, 8, tile), jnp.float32),
                vmem((TILES, 8, tile), jnp.float32),
                vmem((4, 3) + flat, jnp.float32),
                vmem((16, 3) + flat, jnp.float32),
                dma((60,)), dma((64,)), dma((4 * n_chunks,)), dma((4 * n_chunks,)), dma((n_chunks,)),
                dma((4,)), dma((4,)), dma, dma((16,)), dma((16,)), dma((8,)),
            ],
            compiler_params=pltpu.CompilerParams(has_side_effects=True, vmem_limit_bytes=66_000_000),
            name="head",
        )(h_part, w_part, draft_loc.reshape(SUBS, 1, tile), q_loc.reshape(flat))
        return lp.reshape(rows), acc.reshape(rows)

    return jax.shard_map(
        per_device, mesh=mesh, in_specs=(P("data", "model"), P("model", "data"), P("data"), P("data")),
        out_specs=(P("data"), P("data")), check_vma=False)


def solution(mesh):
    return build(mesh, 400)
```

```python
import functools

import jax
import jax.numpy as jnp
from jax import lax
from jax.experimental import pallas as pl
from jax.experimental.pallas import tpu as pltpu
from jax.sharding import PartitionSpec as P

MESH = pl.DeviceIdType.MESH
SUBS = 4
TILES = 16
FLOOR = float(jnp.finfo(jnp.float32).min)
LINK_ORDER = ("H0", "H1", "W0", "W1", "W2", "F0", "F1", "H2", "H3", "W3", "W4", "F2", "F3", "W5", "W6", "W7")
H_TIME, W_TIME, STEP_TIME, EARLY_TIME, LAG = 34.3, 422.0, 2.25, 8.0, 3.0
MAX_RUN = 3


def tile_of(q):
    if q < 4:
        return 0, q
    if q < 12:
        return 1 + q % 2, (q - 4) // 2
    return 3, q - 12


def link_order(n_chunks):
    tokens = [(t[0], int(t[1:])) for t in LINK_ORDER]
    last = max(k for kind, k in tokens if kind == "W")
    tokens = [t for t in tokens if t[0] != "W" or t[1] < n_chunks] + [("W", j) for j in range(last + 1, n_chunks)]
    start, after = [], [[], [], [], []]
    current = start
    for kind, k in tokens:
        if kind == "F":
            current = after[k // 2 * 2 + 1]
        current.append((kind, k))
    return start, after


def stretches(values):
    out, i = [], 0
    while i < len(values):
        n = 1
        while n < MAX_RUN and i + n < len(values) and values[i + n] == values[i] + n:
            n += 1
        out.append((n, values[i]))
        i += n
    return out


def plan(sizes):
    start, after = link_order(len(sizes))
    free, done, at = {"x": 0.0, "y": 0.0, "z": 0.0}, {}, {}
    tiles, chunks, cells, runs, pending, new = [], [], set(), [], [], []
    n_main = len(sizes) - 1

    def put(link, token, now):
        free[link] = max(free[link], now) + (W_TIME * sizes[token[1]] / sum(sizes) if token[0] == "W" else H_TIME)
        done[link, token] = free[link]

    def put_x(q, now):
        put("x", ("X", q), now)
        at["x", q] = free["x"] + LAG

    def issue(token, now):
        kind, k = token
        for link in "yz" if kind != "F" else "yz"[k % 2]:
            put(link, token, now)
        if kind == "F":
            at["diag", k] = done["yz"[k % 2], token] + LAG
        else:
            at["yz" if kind == "H" else "w", k] = max(done["y", token], done["z", token]) + LAG

    def handle(e, now):
        kind, k = e
        del at[e]
        pending.append(e)
        if kind == "x":
            at["h", k] = now + LAG
        elif kind == "h":
            new.append(k)
        elif kind == "yz":
            put_x(4 + 2 * k, now)
            put_x(5 + 2 * k, now)
            for token in after[k]:
                issue(token, now)
        elif kind == "diag":
            put_x(12 + k, now)
        elif k < n_main:
            chunks.append(k)

    def first():
        return min(at, key=lambda e: (at[e], e))

    for token in start:
        issue(token, 0.0)
    for q in range(4):
        put_x(q, 0.0)
    now = 0.0
    last_step = 0.0
    while len(cells) < TILES * n_main:
        while at and at[first()] <= now and len(new) < 2:
            handle(first(), now)
        options = [
            (n, (0, q, 0, j, 1, n)) for q in sorted(tiles)
            for n, j in stretches([j for j in sorted(chunks) if (q, j) not in cells])]
        options += [
            (n, (0, q, 1, j, 0, n)) for j in sorted(chunks)
            for n, q in stretches([q for q in sorted(tiles) if (q, j) not in cells])]
        if new:
            run = (1, new.pop(0), 0, 0, 0, 1)
            tiles.append(run[1])
            now += last_step
            last_step = EARLY_TIME
        elif options:
            _, run = max(options, key=lambda o: o[0])
            _, q, dq, j, dj, n = run
            cells.update((q + dq * i, j + dj * i) for i in range(n))
            now += last_step + (n - 1) * STEP_TIME
            last_step = STEP_TIME
        else:
            e = first()
            now = max(now, at[e])
            handle(e, now)
            continue
        runs.append((pending[:], run))
        pending.clear()
    now += last_step
    while at:
        handle(first(), now)
    return runs, pending, now


def kernel(
    v_tile, h_ref, w_ref, ids_ref, q_ref, lp_ref, acc_ref, hbuf, early,
    wv, hv, he, staged, pin, lg, lg_end, ids_all, mx, sm, pk, st_send, st_recv,
    ss, rs, wss, wrs, wls, iss, irs, ils, sss, srs, lsem, hsem, esem, psem,
):
    rows, kp = h_ref.shape
    tile = rows // SUBS
    vocab = w_ref.shape[0]
    share = vocab // 4
    n_chunks = -(-share // v_tile)
    sizes = [min(v_tile, share - j * v_tile) for j in range(n_chunks)]
    runs, leftover, _ = plan(sizes)
    send_first, send_after = link_order(n_chunks)

    d, m = lax.axis_index("data"), lax.axis_index("model")
    y, z = lax.rem(d, 2), d // 2
    core, x = lax.rem(m, 2), m // 2
    m_sib = m + 1 - 2 * core
    m_x = m + 2 - 4 * x
    m_xs = m_sib + 2 - 4 * x

    def block(rb):
        ry, rz = rb % 2, rb // 2
        yy = 1 - y if ry else y
        zz = 1 - z if rz else z
        return zz * 2 + yy

    def row0(q):
        rb, sub = tile_of(q)
        return pl.multiple_of(block(rb) * rows + sub * tile, tile)

    def own_piece(q):
        rb, sub = tile_of(q)
        return h_ref.at[pl.ds(sub * tile, tile), :] if rb == 0 else hbuf.at[m, pl.ds(row0(q), tile), :]

    def send_h(src, q_here, q_there, mm, dev, sem):
        return pltpu.make_async_remote_copy(
            src_ref=src, dst_ref=hbuf.at[mm, pl.ds(row0(q_here), tile), :], send_sem=ss.at[sem],
            recv_sem=rs.at[q_there * 4 + mm], device_id=dev, device_id_type=MESH)

    def wait_h(q, mm):
        pltpu.make_async_remote_copy(
            src_ref=hbuf.at[mm, pl.ds(row0(q), tile), :], dst_ref=hbuf.at[mm, pl.ds(row0(q), tile), :],
            send_sem=ss.at[0], recv_sem=rs.at[q * 4 + mm], device_id=(d, m), device_id_type=MESH).wait_recv()

    def send_w(j, rb):
        size, dd = sizes[j], block(rb)
        return pltpu.make_async_remote_copy(
            src_ref=w_ref.at[pl.ds(pl.multiple_of(dd * share + j * v_tile, 8), size), :],
            dst_ref=wv.at[pl.ds(j * v_tile, size), pl.ds(rb * kp, kp)],
            send_sem=wss.at[j * 4 + rb], recv_sem=wrs.at[j * 4 + rb], device_id=(dd, m), device_id_type=MESH)

    def wait_w(j, rb):
        size = sizes[j]
        pltpu.make_async_remote_copy(
            src_ref=w_ref.at[pl.ds(0, size), :],
            dst_ref=wv.at[pl.ds(j * v_tile, size), pl.ds(rb * kp, kp)],
            send_sem=wss.at[j * 4 + rb], recv_sem=wrs.at[j * 4 + rb], device_id=(d, m), device_id_type=MESH).wait_recv()

    def local_w(j):
        size = sizes[j]
        return pltpu.make_async_copy(
            w_ref.at[pl.ds(pl.multiple_of(d * share + j * v_tile, 8), size), :],
            wv.at[pl.ds(j * v_tile, size), pl.ds(0, kp)], wls.at[j])

    def send_ids(rb):
        return pltpu.make_async_remote_copy(
            src_ref=ids_ref, dst_ref=ids_all.at[rb], send_sem=iss.at[rb], recv_sem=irs.at[rb],
            device_id=(block(rb), m), device_id_type=MESH)

    def put(kind, k):
        if kind == "H":
            send_h(own_piece(k), k, 4 + 2 * k, m, (block(1), m), 48 + k).start()
            send_h(own_piece(k), k, 5 + 2 * k, m, (block(2), m), 52 + k).start()
        elif kind == "F":
            q = 5 + 2 * k if k % 2 == 0 else 4 + 2 * k
            send_h(own_piece(q), q, 12 + k, m, (block(1 + k % 2), m), 56 + k).start()
        else:
            for rb in (3, 1, 2):
                send_w(k, rb).start()

    def spread(q):
        send_h(own_piece(q), q, q, m, (d, m_x), q).start()
        send_h(own_piece(q), q, q, m, (d, m_sib), 16 + q).start()

    def event(kind, k):
        if kind == "x":
            wait_h(k, m_x)
            send_h(hbuf.at[m_x, pl.ds(row0(k), tile), :], k, k, m_x, (d, m_sib), 32 + k).start()
        elif kind == "h":
            wait_h(k, m_sib)
            wait_h(k, m_xs)
            load_piece(jnp.int32(k), 0, he.at[k % 2], hsem.at[k % 2])
        elif kind == "yz":
            wait_h(4 + 2 * k, m)
            wait_h(5 + 2 * k, m)
            spread(4 + 2 * k)
            spread(5 + 2 * k)
            for token in send_after[k]:
                put(*token)
        elif kind == "diag":
            wait_h(12 + k, m)
            spread(12 + k)
        else:
            for rb in (1, 2, 3):
                wait_w(k, rb)

    def rb_sub(q):
        mid = q >= 4
        late = q >= 12
        rb = jnp.where(late, 3, jnp.where(mid, 1 + lax.rem(q, 2), 0))
        sub = jnp.where(late, q - 12, jnp.where(mid, (q - 4) // 2, q))
        return rb, sub

    def load_piece(q, part, dst, sem):
        rb, sub = rb_sub(q)
        ry, rz = lax.rem(rb, 2), rb // 2
        yy, zz = y + ry - 2 * y * ry, z + rz - 2 * z * rz
        row = pl.multiple_of((zz * 2 + yy) * rows + sub * tile, tile)
        mm = block(part)
        mine = jnp.logical_and(rb == 0, mm == m)

        @pl.when(mine)
        def _():
            pltpu.make_async_copy(h_ref.at[pl.ds(pl.multiple_of(sub * tile, tile), tile), :], dst, sem).start()

        @pl.when(jnp.logical_not(mine))
        def _():
            pltpu.make_async_copy(hbuf.at[mm, pl.ds(row, tile), :], dst, sem).start()

    def load_parts(q, slot):
        for part in (1, 2, 3):
            load_piece(q, part, hv.at[slot, :, pl.ds((part - 1) * kp, kp)], lsem.at[slot * 4 + part])

    def wait_parts(slot):
        for part in (1, 2, 3):
            pltpu.make_async_copy(
                h_ref.at[pl.ds(0, tile), :], hv.at[slot, :, pl.ds((part - 1) * kp, kp)], lsem.at[slot * 4 + part]).wait()

    def early_out(q, start, size, slot):
        return pltpu.make_async_copy(staged.at[slot, pl.ds(0, size), :], early.at[q, pl.ds(start, size), :], esem.at[slot])

    def early_in(q, start, size, slot):
        return pltpu.make_async_copy(early.at[q, pl.ds(start, size), :], pin.at[slot, pl.ds(0, size), :], psem.at[slot])

    own_ids = pltpu.make_async_copy(ids_ref, ids_all.at[0], ils)
    own_ids.start()
    for rb in (1, 2, 3):
        send_ids(rb).start()
    for i, token in enumerate(send_first):
        put(*token)
        if i == 0:
            for q in range(4):
                spread(q)
    for j in range(n_chunks):
        local_w(j).start()
    mx[...] = jnp.full(mx.shape, FLOOR, jnp.float32)
    sm[...] = jnp.zeros(sm.shape, jnp.float32)
    pk[...] = jnp.zeros(pk.shape, jnp.float32)
    lg[...] = jnp.full(lg.shape, -jnp.inf, jnp.float32)
    lg_end[...] = jnp.full(lg_end.shape, -jnp.inf, jnp.float32)
    own_ids.wait()
    for rb in (1, 2, 3):
        send_ids(rb).wait()
    for j in range(n_chunks):
        local_w(j).wait()

    base = m * vocab + d * share
    nowhere = jnp.int32(1 << 30)

    def dot(a, b):
        return lax.dot_general(a, b, (((1,), (1,)), ((), ())), preferred_element_type=jnp.float32)

    def product(start, size, slot, pslot):
        return dot(wv[pl.ds(start, size), kp:], hv[slot]) + pin[pslot, :size]

    end_start, end_size = (n_chunks - 1) * v_tile, sizes[-1]

    def early_products(q):
        half = lax.rem(q, 2)
        pltpu.make_async_copy(h_ref.at[pl.ds(0, tile), :], he.at[half], hsem.at[half]).wait()

        def one(j, carry):
            slot = lax.rem(j, 2)
            start = pl.multiple_of(j * v_tile, 8)
            pl.when(j >= 2)(lambda: early_out(q, start, v_tile, slot).wait())
            staged[slot] = dot(wv[pl.ds(start, v_tile), :kp], he[half])
            early_out(q, start, v_tile, slot).start()
            return carry

        lax.fori_loop(0, n_chunks - 1, one, 0)
        slot = (n_chunks - 1) % 2
        early_out(q, 0, v_tile, slot).wait()
        staged[slot, :end_size] = dot(wv[end_start:end_start + end_size, :kp], he[half])
        early_out(q, end_start, end_size, slot).start()
        early_out(q, 0, v_tile, 1 - slot).wait()
        early_out(q, end_start, end_size, slot).wait()

    def absorb(ref, q, start):
        rb, sub = rb_sub(q)
        size = ref.shape[0]
        spot = ids_all[rb, sub] - (base + start) - lax.broadcasted_iota(jnp.int32, (8, tile), 0)
        old = mx[q]
        new = old
        for k in range(0, size, 8):
            new = jnp.maximum(new, ref[k:k + 8, :])
        grown, picked = sm[q] * jnp.exp(old - new), pk[q]
        for k in range(0, size, 8):
            part = ref[k:k + 8, :]
            grown = grown + jnp.exp(part - new)
            picked = picked + jnp.where(spot == k, part, 0.0)
        mx[q] = new
        sm[q] = grown
        pk[q] = picked

    n_runs = len(runs)
    held, codes = TILES - 1, []
    for i, (_, (kind, q0, dq, j0, dj, n)) in enumerate(runs):
        following = runs[i + 1][1] if i + 1 < n_runs else (2, 0, 0, 0, 0, 1)
        held = q0 + dq * (n - 1) if kind == 0 else held
        q_next = held if following[0] == 1 else following[1]
        held = q_next
        code = 0
        for digit, radix in (
            (kind, 2), (q0, 16), (dq, 2), (j0, 8), (dj, 2), (n, 8), (q_next, 16), (following[3], 8), (following[0] == 0, 2)):
            code = code * radix + int(digit)
        codes.append(code)

    for e in runs[0][0]:
        event(*e)

    def run_body(r, carry):
        code = jnp.int32(codes[0])
        for i in range(1, n_runs):
            code = jnp.where(r >= i, jnp.int32(codes[i]), code)
        digits = []
        for radix in (2, 8, 16, 8, 2, 8, 2, 16, 2):
            digits.append(lax.rem(code, radix))
            code = code // radix
        next_main, j_next, q_next, n, dj, j0, dq, q0, kind = digits

        def step(i, carry):
            slot, fresh, held, pslot, q_old, start_old = carry
            q, j = q0 + dq * i, j0 + dj * i
            last = i == n - 1

            @pl.when(last)
            def _():
                for k in range(1, n_runs):
                    if runs[k][0]:
                        @pl.when(r == k - 1)
                        def _(k=k):
                            for e in runs[k][0]:
                                event(*e)

            q_new, j_new = jnp.where(last, q_next, q + dq), jnp.where(last, j_next, j + dj)
            more = jnp.where(last, next_main, 1) == 1
            after = pl.multiple_of(j_new * v_tile, 8)
            start = pl.multiple_of(j * v_tile, 8)
            pl.when(q_new != held)(lambda: load_parts(q_new, 1 - slot))

            @pl.when(kind == 1)
            def _():
                early_products(q)
                pl.when(more)(lambda: early_in(q_new, after, v_tile, pslot).start())

            @pl.when(kind == 0)
            def _():
                pl.when(more)(lambda: early_in(q_new, after, v_tile, 1 - pslot).start())
                pl.when(fresh == 1)(lambda: wait_parts(slot))
                early_in(q, start, v_tile, pslot).wait()
                absorb(lg, q_old, start_old)
                lg[...] = product(start, v_tile, slot, pslot)

            load = q_new != held
            main = kind == 0
            return (
                jnp.where(load, 1 - slot, slot), jnp.where(load, 1, jnp.where(main, 0, fresh)), q_new,
                jnp.where(main, 1 - pslot, pslot), jnp.where(main, q, q_old), jnp.where(main, start, start_old))

        return lax.fori_loop(0, n, step, carry)

    zero = jnp.int32(0)
    slot, fresh, _, pslot, q_old, start_old = lax.fori_loop(
        0, n_runs, run_body, (zero, zero, jnp.int32(TILES - 1), zero, zero, nowhere))

    early_in(0, end_start, end_size, pslot).start()
    absorb(lg, q_old, start_old)
    for e in leftover:
        event(*e)

    def end_step(q, carry):
        slot, fresh, pslot, q_old, start_old = carry

        @pl.when(q < TILES - 1)
        def _():
            load_parts(q + 1, 1 - slot)
            early_in(q + 1, end_start, end_size, 1 - pslot).start()

        pl.when(fresh == 1)(lambda: wait_parts(slot))
        early_in(q, end_start, end_size, pslot).wait()
        absorb(lg_end, q_old, start_old)
        lg_end[...] = product(end_start, end_size, slot, pslot)
        return 1 - slot, jnp.int32(1), 1 - pslot, q, jnp.int32(end_start)

    _, _, _, q_old, start_old = lax.fori_loop(0, TILES, end_step, (slot, fresh, pslot, zero, nowhere))
    absorb(lg_end, q_old, start_old)

    lanes = 128
    for q in range(TILES):
        rb, sub = tile_of(q)
        old = mx[q]
        top = jnp.max(old, axis=0, keepdims=True)
        parts = (top, jnp.sum(sm[q] * jnp.exp(old - top), axis=0, keepdims=True), jnp.sum(pk[q], axis=0, keepdims=True))
        for k, part in enumerate(parts):
            for i in range(tile // lanes):
                st_send[rb, k, pl.ds(sub * (tile // lanes) + i, 1), :] = part[:, i * lanes:(i + 1) * lanes]

    me = d * 4 + m
    st_recv[me] = st_send[0]

    def send_stats(rb, o):
        return pltpu.make_async_remote_copy(
            src_ref=st_send.at[rb], dst_ref=st_recv.at[me], send_sem=sss.at[rb * 4 + o], recv_sem=srs.at[me],
            device_id=(block(rb), lax.rem(m + o, 4)), device_id_type=MESH)

    others = [(rb, o) for rb in (3, 2, 1, 0) for o in range(4) if (rb, o) != (0, 0)]
    for rb, o in others:
        send_stats(rb, o).start()

    def drain(i, carry):
        pltpu.make_async_remote_copy(
            src_ref=h_ref.at[pl.ds(0, tile), :], dst_ref=hbuf.at[0, pl.ds(0, tile), :], send_sem=ss.at[i],
            recv_sem=rs.at[0], device_id=(d, m), device_id_type=MESH).wait_send()
        return carry

    lax.fori_loop(0, 60, drain, 0)
    for j in range(n_chunks):
        for rb in (1, 2, 3):
            send_w(j, rb).wait_send()
    for rb, o in others:
        send_stats(rb, o).wait_send()
    for rb, o in others:
        source = block(rb) * 4 + lax.rem(m + o, 4)
        pltpu.make_async_remote_copy(
            src_ref=st_send.at[rb], dst_ref=st_recv.at[source], send_sem=sss.at[rb * 4 + o], recv_sem=srs.at[source],
            device_id=(d, m), device_id_type=MESH).wait_recv()

    top = jnp.max(st_recv[:, 0], axis=0)
    total = jnp.sum(st_recv[:, 1] * jnp.exp(st_recv[:, 0] - top[None]), axis=0)
    picked = jnp.sum(st_recv[:, 2], axis=0)
    log_prob = picked - (top + jnp.log(total))
    lp_ref[...] = log_prob
    acc_ref[...] = jnp.minimum(1.0, jnp.exp(log_prob) / q_ref[...])


def build(mesh, v_tile):
    def per_device(h_part, w_part, draft_loc, q_loc):
        rows, kp = h_part.shape
        vocab = w_part.shape[0]
        share, tile = vocab // 4, rows // SUBS
        n_chunks = -(-share // v_tile)
        lanes = 128
        flat = (rows // lanes, lanes)
        dma, vmem = pltpu.SemaphoreType.DMA, pltpu.VMEM
        any_space = pl.BlockSpec(memory_space=pl.ANY)
        in_vmem = pl.BlockSpec(memory_space=pltpu.VMEM)
        lp, acc, _, _ = pl.pallas_call(
            functools.partial(kernel, v_tile),
            out_shape=(
                jax.ShapeDtypeStruct(flat, jnp.float32),
                jax.ShapeDtypeStruct(flat, jnp.float32),
                jax.ShapeDtypeStruct((4, 4 * rows, kp), jnp.bfloat16),
                jax.ShapeDtypeStruct((TILES, share, tile), jnp.float32),
            ),
            in_specs=[any_space, any_space, in_vmem, in_vmem],
            out_specs=(in_vmem, in_vmem, any_space, any_space),
            scratch_shapes=[
                vmem((share, 4 * kp), jnp.bfloat16),
                vmem((2, tile, 3 * kp), jnp.bfloat16),
                vmem((2, tile, kp), jnp.bfloat16),
                vmem((2, v_tile, tile), jnp.float32),
                vmem((2, v_tile, tile), jnp.float32),
                vmem((v_tile, tile), jnp.float32),
                vmem((share - (n_chunks - 1) * v_tile, tile), jnp.float32),
                vmem((4, SUBS, 1, tile), jnp.int32),
                vmem((TILES, 8, tile), jnp.float32),
                vmem((TILES, 8, tile), jnp.float32),
                vmem((TILES, 8, tile), jnp.float32),
                vmem((4, 3) + flat, jnp.float32),
                vmem((16, 3) + flat, jnp.float32),
                dma((60,)), dma((64,)), dma((4 * n_chunks,)), dma((4 * n_chunks,)), dma((n_chunks,)),
                dma((4,)), dma((4,)), dma, dma((16,)), dma((16,)), dma((8,)), dma((2,)), dma((2,)), dma((2,)),
            ],
            compiler_params=pltpu.CompilerParams(has_side_effects=True, vmem_limit_bytes=66_000_000),
            name="head",
        )(h_part, w_part, draft_loc.reshape(SUBS, 1, tile), q_loc.reshape(flat))
        return lp.reshape(rows), acc.reshape(rows)

    return jax.shard_map(
        per_device, mesh=mesh, in_specs=(P("data", "model"), P("model", "data"), P("data"), P("data")),
        out_specs=(P("data"), P("data")), check_vma=False)


def solution(mesh):
    return build(mesh, 400)
```

```python
import functools

import jax
import jax.numpy as jnp
from jax import lax
from jax.experimental import pallas as pl
from jax.experimental.pallas import tpu as pltpu
from jax.sharding import PartitionSpec as P

MESH = pl.DeviceIdType.MESH
SUBS = 4
TILES = 16
FLOOR = float(jnp.finfo(jnp.float32).min)
LINK_ORDER = ("H0", "W0", "W1", "H1", "W2", "H2", "F0", "F1", "W3", "H3", "W4", "F2", "F3", "W5", "W6", "W7")
H_TIME, W_TIME, STEP_TIME, EARLY_TIME, LAG = 33.9, 417.0, 2.4, 8.7, 3.0
MAX_RUN = 3


def tile_of(q):
    if q < 4:
        return 0, q
    if q < 12:
        return 1 + q % 2, (q - 4) // 2
    return 3, q - 12


def link_order(n_chunks):
    tokens = [(t[0], int(t[1:])) for t in LINK_ORDER]
    last = max(k for kind, k in tokens if kind == "W")
    tokens = [t for t in tokens if t[0] != "W" or t[1] < n_chunks] + [("W", j) for j in range(last + 1, n_chunks)]
    start, after = [], [[], [], [], []]
    current = start
    for kind, k in tokens:
        if kind == "F":
            current = after[k // 2 * 2 + 1]
        current.append((kind, k))
    return start, after


def stretches(values):
    out, i = [], 0
    while i < len(values):
        n = 1
        while n < MAX_RUN and i + n < len(values) and values[i + n] == values[i] + n:
            n += 1
        out.append((n, values[i]))
        i += n
    return out


def plan(sizes):
    start, after = link_order(len(sizes))
    free, done, at = {"x": 0.0, "y": 0.0, "z": 0.0}, {}, {}
    tiles, chunks, cells, runs, pending, new = [], [], set(), [], [], []
    n_main = len(sizes) - 1

    def put(link, token, now):
        free[link] = max(free[link], now) + (W_TIME * sizes[token[1]] / sum(sizes) if token[0] == "W" else H_TIME)
        done[link, token] = free[link]

    def put_x(q, now):
        put("x", ("X", q), now)
        at["x", q] = free["x"] + LAG

    def issue(token, now):
        kind, k = token
        for link in "yz" if kind != "F" else "yz"[k % 2]:
            put(link, token, now)
        if kind == "F":
            at["diag", k] = done["yz"[k % 2], token] + LAG
        else:
            at["yz" if kind == "H" else "w", k] = max(done["y", token], done["z", token]) + LAG

    def handle(e, now):
        kind, k = e
        del at[e]
        pending.append(e)
        if kind == "x":
            at["h", k] = now + LAG
        elif kind == "h":
            new.append(k)
        elif kind == "yz":
            put_x(4 + 2 * k, now)
            put_x(5 + 2 * k, now)
            for token in after[k]:
                issue(token, now)
        elif kind == "diag":
            put_x(12 + k, now)
        elif k < n_main:
            chunks.append(k)

    def first():
        return min(at, key=lambda e: (at[e], e))

    for token in start:
        issue(token, 0.0)
    for q in range(4):
        put_x(q, 0.0)
    now = 0.0
    last_step = 0.0
    while len(cells) < TILES * n_main:
        while at and at[first()] <= now and len(new) < 2:
            handle(first(), now)
        options = [
            (n if n == 1 else n + 1.5, (0, q, 0, j, 1, n)) for q in sorted(tiles)
            for n, j in stretches([j for j in sorted(chunks) if (q, j) not in cells])]
        options += [
            (n, (0, q, 1, j, 0, n)) for j in sorted(chunks)
            for n, q in stretches([q for q in sorted(tiles) if (q, j) not in cells])]
        if new:
            run = (1, new.pop(0), 0, 0, 0, 1)
            tiles.append(run[1])
            now += last_step
            last_step = EARLY_TIME
        elif options:
            _, run = max(options, key=lambda o: o[0])
            _, q, dq, j, dj, n = run
            cells.update((q + dq * i, j + dj * i) for i in range(n))
            now += last_step + (n - 1) * STEP_TIME
            last_step = STEP_TIME
        else:
            e = first()
            now = max(now, at[e])
            handle(e, now)
            continue
        runs.append((pending[:], run))
        pending.clear()
    now += last_step
    while at:
        handle(first(), now)
    return runs, pending, now


def kernel(
    v_tile, h_ref, w_ref, ids_ref, q_ref, lp_ref, acc_ref, hbuf, early,
    wv, hv, he, staged, pin, lg, lg_end, ids_all, mx, sm, pk, st_send, st_recv,
    ss, rs, wss, wrs, wls, iss, irs, ils, sss, srs, lsem, hsem, esem, psem,
):
    rows, kp = h_ref.shape
    tile = rows // SUBS
    vocab = w_ref.shape[0]
    share = vocab // 4
    n_chunks = -(-share // v_tile)
    sizes = [min(v_tile, share - j * v_tile) for j in range(n_chunks)]
    runs, leftover, _ = plan(sizes)
    send_first, send_after = link_order(n_chunks)

    d, m = lax.axis_index("data"), lax.axis_index("model")
    y, z = lax.rem(d, 2), d // 2
    core, x = lax.rem(m, 2), m // 2
    m_sib = m + 1 - 2 * core
    m_x = m + 2 - 4 * x
    m_xs = m_sib + 2 - 4 * x

    def block(rb):
        ry, rz = rb % 2, rb // 2
        yy = 1 - y if ry else y
        zz = 1 - z if rz else z
        return zz * 2 + yy

    def row0(q):
        rb, sub = tile_of(q)
        return pl.multiple_of(block(rb) * rows + sub * tile, tile)

    def own_piece(q):
        rb, sub = tile_of(q)
        return h_ref.at[pl.ds(sub * tile, tile), :] if rb == 0 else hbuf.at[m, pl.ds(row0(q), tile), :]

    def send_h(src, q_here, q_there, mm, dev, sem):
        return pltpu.make_async_remote_copy(
            src_ref=src, dst_ref=hbuf.at[mm, pl.ds(row0(q_here), tile), :], send_sem=ss.at[sem],
            recv_sem=rs.at[q_there * 4 + mm], device_id=dev, device_id_type=MESH)

    def wait_h(q, mm):
        pltpu.make_async_remote_copy(
            src_ref=hbuf.at[mm, pl.ds(row0(q), tile), :], dst_ref=hbuf.at[mm, pl.ds(row0(q), tile), :],
            send_sem=ss.at[0], recv_sem=rs.at[q * 4 + mm], device_id=(d, m), device_id_type=MESH).wait_recv()

    def send_w(j, rb):
        size, dd = sizes[j], block(rb)
        return pltpu.make_async_remote_copy(
            src_ref=w_ref.at[pl.ds(pl.multiple_of(dd * share + j * v_tile, 8), size), :],
            dst_ref=wv.at[pl.ds(j * v_tile, size), pl.ds(rb * kp, kp)],
            send_sem=wss.at[j * 4 + rb], recv_sem=wrs.at[j * 4 + rb], device_id=(dd, m), device_id_type=MESH)

    def wait_w(j, rb):
        size = sizes[j]
        pltpu.make_async_remote_copy(
            src_ref=w_ref.at[pl.ds(0, size), :],
            dst_ref=wv.at[pl.ds(j * v_tile, size), pl.ds(rb * kp, kp)],
            send_sem=wss.at[j * 4 + rb], recv_sem=wrs.at[j * 4 + rb], device_id=(d, m), device_id_type=MESH).wait_recv()

    def local_w(j):
        size = sizes[j]
        return pltpu.make_async_copy(
            w_ref.at[pl.ds(pl.multiple_of(d * share + j * v_tile, 8), size), :],
            wv.at[pl.ds(j * v_tile, size), pl.ds(0, kp)], wls.at[j])

    def send_ids(rb):
        return pltpu.make_async_remote_copy(
            src_ref=ids_ref, dst_ref=ids_all.at[rb], send_sem=iss.at[rb], recv_sem=irs.at[rb],
            device_id=(block(rb), m), device_id_type=MESH)

    def put(kind, k):
        if kind == "H":
            send_h(own_piece(k), k, 4 + 2 * k, m, (block(1), m), 48 + k).start()
            send_h(own_piece(k), k, 5 + 2 * k, m, (block(2), m), 52 + k).start()
        elif kind == "F":
            q = 5 + 2 * k if k % 2 == 0 else 4 + 2 * k
            send_h(own_piece(q), q, 12 + k, m, (block(1 + k % 2), m), 56 + k).start()
        else:
            for rb in (3, 1, 2):
                send_w(k, rb).start()

    def spread(q):
        send_h(own_piece(q), q, q, m, (d, m_x), q).start()
        send_h(own_piece(q), q, q, m, (d, m_sib), 16 + q).start()

    def event(kind, k):
        if kind == "x":
            wait_h(k, m_x)
            send_h(hbuf.at[m_x, pl.ds(row0(k), tile), :], k, k, m_x, (d, m_sib), 32 + k).start()
        elif kind == "h":
            wait_h(k, m_sib)
            wait_h(k, m_xs)
            load_piece(jnp.int32(k), 0, he.at[k % 2], hsem.at[k % 2])
        elif kind == "yz":
            wait_h(4 + 2 * k, m)
            wait_h(5 + 2 * k, m)
            spread(4 + 2 * k)
            spread(5 + 2 * k)
            for token in send_after[k]:
                put(*token)
        elif kind == "diag":
            wait_h(12 + k, m)
            spread(12 + k)
        else:
            for rb in (1, 2, 3):
                wait_w(k, rb)

    def rb_sub(q):
        mid = q >= 4
        late = q >= 12
        rb = jnp.where(late, 3, jnp.where(mid, 1 + lax.rem(q, 2), 0))
        sub = jnp.where(late, q - 12, jnp.where(mid, (q - 4) // 2, q))
        return rb, sub

    def load_piece(q, part, dst, sem):
        rb, sub = rb_sub(q)
        ry, rz = lax.rem(rb, 2), rb // 2
        yy, zz = y + ry - 2 * y * ry, z + rz - 2 * z * rz
        row = pl.multiple_of((zz * 2 + yy) * rows + sub * tile, tile)
        mm = block(part)
        mine = jnp.logical_and(rb == 0, mm == m)

        @pl.when(mine)
        def _():
            pltpu.make_async_copy(h_ref.at[pl.ds(pl.multiple_of(sub * tile, tile), tile), :], dst, sem).start()

        @pl.when(jnp.logical_not(mine))
        def _():
            pltpu.make_async_copy(hbuf.at[mm, pl.ds(row, tile), :], dst, sem).start()

    def load_parts(q, slot):
        for part in (1, 2, 3):
            load_piece(q, part, hv.at[slot, :, pl.ds((part - 1) * kp, kp)], lsem.at[slot * 4 + part])

    def wait_parts(slot):
        for part in (1, 2, 3):
            pltpu.make_async_copy(
                h_ref.at[pl.ds(0, tile), :], hv.at[slot, :, pl.ds((part - 1) * kp, kp)], lsem.at[slot * 4 + part]).wait()

    def early_out(q, start, size, slot):
        return pltpu.make_async_copy(staged.at[slot, pl.ds(0, size), :], early.at[q, pl.ds(start, size), :], esem.at[slot])

    def early_in(q, start, size, slot):
        return pltpu.make_async_copy(early.at[q, pl.ds(start, size), :], pin.at[slot, pl.ds(0, size), :], psem.at[slot])

    own_ids = pltpu.make_async_copy(ids_ref, ids_all.at[0], ils)
    own_ids.start()
    for rb in (1, 2, 3):
        send_ids(rb).start()
    for i, token in enumerate(send_first):
        put(*token)
        if i == 0:
            for q in range(4):
                spread(q)
    for j in range(n_chunks):
        local_w(j).start()
    mx[...] = jnp.full(mx.shape, FLOOR, jnp.float32)
    sm[...] = jnp.zeros(sm.shape, jnp.float32)
    pk[...] = jnp.zeros(pk.shape, jnp.float32)
    lg[...] = jnp.full(lg.shape, -jnp.inf, jnp.float32)
    lg_end[...] = jnp.full(lg_end.shape, -jnp.inf, jnp.float32)
    own_ids.wait()
    for rb in (1, 2, 3):
        send_ids(rb).wait()
    for j in range(n_chunks):
        local_w(j).wait()

    base = m * vocab + d * share
    nowhere = jnp.int32(1 << 30)

    def dot(a, b):
        return lax.dot_general(a, b, (((1,), (1,)), ((), ())), preferred_element_type=jnp.float32)

    def product(start, size, slot, pslot):
        return dot(wv[pl.ds(start, size), kp:], hv[slot]) + pin[pslot, :size]

    end_start, end_size = (n_chunks - 1) * v_tile, sizes[-1]

    def early_products(q):
        half = lax.rem(q, 2)
        pltpu.make_async_copy(h_ref.at[pl.ds(0, tile), :], he.at[half], hsem.at[half]).wait()

        def one(j, carry):
            slot = lax.rem(j, 2)
            start = pl.multiple_of(j * v_tile, 8)
            pl.when(j >= 2)(lambda: early_out(q, start, v_tile, slot).wait())
            staged[slot] = dot(wv[pl.ds(start, v_tile), :kp], he[half])
            early_out(q, start, v_tile, slot).start()
            return carry

        lax.fori_loop(0, n_chunks - 1, one, 0)
        slot = (n_chunks - 1) % 2
        early_out(q, 0, v_tile, slot).wait()
        staged[slot, :end_size] = dot(wv[end_start:end_start + end_size, :kp], he[half])
        early_out(q, end_start, end_size, slot).start()
        early_out(q, 0, v_tile, 1 - slot).wait()
        early_out(q, end_start, end_size, slot).wait()

    def absorb(ref, q, start):
        rb, sub = rb_sub(q)
        size = ref.shape[0]
        spot = ids_all[rb, sub] - (base + start) - lax.broadcasted_iota(jnp.int32, (8, tile), 0)
        old = mx[q]
        new = old
        for k in range(0, size, 8):
            new = jnp.maximum(new, ref[k:k + 8, :])
        grown, picked = sm[q] * jnp.exp(old - new), pk[q]
        for k in range(0, size, 8):
            part = ref[k:k + 8, :]
            grown = grown + jnp.exp(part - new)
            picked = picked + jnp.where(spot == k, part, 0.0)
        mx[q] = new
        sm[q] = grown
        pk[q] = picked

    n_runs = len(runs)
    held, codes = TILES - 1, []
    for i, (_, (kind, q0, dq, j0, dj, n)) in enumerate(runs):
        following = runs[i + 1][1] if i + 1 < n_runs else (2, TILES - 1, 0, 0, 0, 1)
        held = q0 + dq * (n - 1) if kind == 0 else held
        q_next = held if following[0] == 1 else following[1]
        held = q_next
        code = 0
        for digit, radix in (
            (kind, 2), (q0, 16), (dq, 2), (j0, 8), (dj, 2), (n, 8), (q_next, 16), (following[3], 8), (following[0] == 0, 2)):
            code = code * radix + int(digit)
        codes.append(code)

    for e in runs[0][0]:
        event(*e)

    def run_body(r, carry):
        code = jnp.int32(codes[0])
        for i in range(1, n_runs):
            code = jnp.where(r >= i, jnp.int32(codes[i]), code)
        digits = []
        for radix in (2, 8, 16, 8, 2, 8, 2, 16, 2):
            digits.append(lax.rem(code, radix))
            code = code // radix
        next_main, j_next, q_next, n, dj, j0, dq, q0, kind = digits

        def step(i, carry):
            slot, fresh, held, pslot, q_old, start_old = carry
            q, j = q0 + dq * i, j0 + dj * i
            last = i == n - 1

            @pl.when(last)
            def _():
                for k in range(1, n_runs):
                    if runs[k][0]:
                        @pl.when(r == k - 1)
                        def _(k=k):
                            for e in runs[k][0]:
                                event(*e)

            q_new, j_new = jnp.where(last, q_next, q + dq), jnp.where(last, j_next, j + dj)
            more = jnp.where(last, next_main, 1) == 1
            after = pl.multiple_of(j_new * v_tile, 8)
            start = pl.multiple_of(j * v_tile, 8)
            pl.when(q_new != held)(lambda: load_parts(q_new, 1 - slot))

            @pl.when(kind == 1)
            def _():
                early_products(q)
                pl.when(more)(lambda: early_in(q_new, after, v_tile, pslot).start())

            @pl.when(kind == 0)
            def _():
                pl.when(more)(lambda: early_in(q_new, after, v_tile, 1 - pslot).start())
                pl.when(fresh == 1)(lambda: wait_parts(slot))
                early_in(q, start, v_tile, pslot).wait()
                absorb(lg, q_old, start_old)
                lg[...] = product(start, v_tile, slot, pslot)

            load = q_new != held
            main = kind == 0
            return (
                jnp.where(load, 1 - slot, slot), jnp.where(load, 1, jnp.where(main, 0, fresh)), q_new,
                jnp.where(main, 1 - pslot, pslot), jnp.where(main, q, q_old), jnp.where(main, start, start_old))

        return lax.fori_loop(0, n, step, carry)

    zero = jnp.int32(0)
    slot, fresh, _, pslot, q_old, start_old = lax.fori_loop(
        0, n_runs, run_body, (zero, zero, jnp.int32(TILES - 1), zero, zero, nowhere))

    lanes = 128
    me = d * 4 + m

    def finish(rb):
        for q in [q for q in range(TILES) if tile_of(q)[0] == rb]:
            sub = tile_of(q)[1]
            old = mx[q]
            top = jnp.max(old, axis=0, keepdims=True)
            parts = (
                top, jnp.sum(sm[q] * jnp.exp(old - top), axis=0, keepdims=True), jnp.sum(pk[q], axis=0, keepdims=True))
            for k, part in enumerate(parts):
                for i in range(tile // lanes):
                    st_send[rb, k, pl.ds(sub * (tile // lanes) + i, 1), :] = part[:, i * lanes:(i + 1) * lanes]

    def send_stats(rb, o):
        return pltpu.make_async_remote_copy(
            src_ref=st_send.at[rb], dst_ref=st_recv.at[me], send_sem=sss.at[rb * 4 + o], recv_sem=srs.at[me],
            device_id=(block(rb), lax.rem(m + o, 4)), device_id_type=MESH)

    others = [(rb, o) for rb in (3, 2, 1, 0) for o in range(4) if (rb, o) != (0, 0)]

    def send_blocks(*blocks):
        for rb, o in others:
            if rb in blocks:
                send_stats(rb, o).start()

    early_in(TILES - 1, end_start, end_size, pslot).start()
    absorb(lg, q_old, start_old)
    for e in leftover:
        event(*e)

    def end_step(i, carry):
        slot, fresh, pslot, q_old, start_old = carry
        q = TILES - 1 - i

        @pl.when(q > 0)
        def _():
            load_parts(q - 1, 1 - slot)
            early_in(q - 1, end_start, end_size, 1 - pslot).start()

        pl.when(q == 10)(lambda: finish(3))
        pl.when(q == 9)(lambda: send_blocks(3))
        pl.when(q == 2)(lambda: [finish(1), finish(2)] and None)
        pl.when(q == 1)(lambda: send_blocks(2, 1))
        pl.when(fresh == 1)(lambda: wait_parts(slot))
        early_in(q, end_start, end_size, pslot).wait()
        absorb(lg_end, q_old, start_old)
        lg_end[...] = product(end_start, end_size, slot, pslot)
        return 1 - slot, jnp.int32(1), 1 - pslot, q, jnp.int32(end_start)

    _, _, _, q_old, start_old = lax.fori_loop(0, TILES, end_step, (slot, fresh, pslot, jnp.int32(TILES - 1), nowhere))
    absorb(lg_end, q_old, start_old)
    finish(0)

    def drain(i, carry):
        pltpu.make_async_remote_copy(
            src_ref=h_ref.at[pl.ds(0, tile), :], dst_ref=hbuf.at[0, pl.ds(0, tile), :], send_sem=ss.at[i],
            recv_sem=rs.at[0], device_id=(d, m), device_id_type=MESH).wait_send()
        return carry

    lax.fori_loop(0, 60, drain, 0)
    for j in range(n_chunks):
        for rb in (1, 2, 3):
            send_w(j, rb).wait_send()
    st_recv[me] = st_send[0]
    send_blocks(0)
    for rb, o in others:
        send_stats(rb, o).wait_send()
    for rb, o in others:
        source = block(rb) * 4 + lax.rem(m + o, 4)
        pltpu.make_async_remote_copy(
            src_ref=st_send.at[rb], dst_ref=st_recv.at[source], send_sem=sss.at[rb * 4 + o], recv_sem=srs.at[source],
            device_id=(d, m), device_id_type=MESH).wait_recv()

    top = jnp.max(st_recv[:, 0], axis=0)
    total = jnp.sum(st_recv[:, 1] * jnp.exp(st_recv[:, 0] - top[None]), axis=0)
    picked = jnp.sum(st_recv[:, 2], axis=0)
    log_prob = picked - (top + jnp.log(total))
    lp_ref[...] = log_prob
    acc_ref[...] = jnp.minimum(1.0, jnp.exp(log_prob) / q_ref[...])


def build(mesh, v_tile):
    def per_device(h_part, w_part, draft_loc, q_loc):
        rows, kp = h_part.shape
        vocab = w_part.shape[0]
        share, tile = vocab // 4, rows // SUBS
        n_chunks = -(-share // v_tile)
        lanes = 128
        flat = (rows // lanes, lanes)
        dma, vmem = pltpu.SemaphoreType.DMA, pltpu.VMEM
        any_space = pl.BlockSpec(memory_space=pl.ANY)
        in_vmem = pl.BlockSpec(memory_space=pltpu.VMEM)
        lp, acc, _, _ = pl.pallas_call(
            functools.partial(kernel, v_tile),
            out_shape=(
                jax.ShapeDtypeStruct(flat, jnp.float32),
                jax.ShapeDtypeStruct(flat, jnp.float32),
                jax.ShapeDtypeStruct((4, 4 * rows, kp), jnp.bfloat16),
                jax.ShapeDtypeStruct((TILES, share, tile), jnp.float32),
            ),
            in_specs=[any_space, any_space, in_vmem, in_vmem],
            out_specs=(in_vmem, in_vmem, any_space, any_space),
            scratch_shapes=[
                vmem((share, 4 * kp), jnp.bfloat16),
                vmem((2, tile, 3 * kp), jnp.bfloat16),
                vmem((2, tile, kp), jnp.bfloat16),
                vmem((2, v_tile, tile), jnp.float32),
                vmem((2, v_tile, tile), jnp.float32),
                vmem((v_tile, tile), jnp.float32),
                vmem((share - (n_chunks - 1) * v_tile, tile), jnp.float32),
                vmem((4, SUBS, 1, tile), jnp.int32),
                vmem((TILES, 8, tile), jnp.float32),
                vmem((TILES, 8, tile), jnp.float32),
                vmem((TILES, 8, tile), jnp.float32),
                vmem((4, 3) + flat, jnp.float32),
                vmem((16, 3) + flat, jnp.float32),
                dma((60,)), dma((64,)), dma((4 * n_chunks,)), dma((4 * n_chunks,)), dma((n_chunks,)),
                dma((4,)), dma((4,)), dma, dma((16,)), dma((16,)), dma((8,)), dma((2,)), dma((2,)), dma((2,)),
            ],
            compiler_params=pltpu.CompilerParams(has_side_effects=True, vmem_limit_bytes=66_000_000),
            name="head",
        )(h_part, w_part, draft_loc.reshape(SUBS, 1, tile), q_loc.reshape(flat))
        return lp.reshape(rows), acc.reshape(rows)

    return jax.shard_map(
        per_device, mesh=mesh, in_specs=(P("data", "model"), P("model", "data"), P("data"), P("data")),
        out_specs=(P("data"), P("data")), check_vma=False)


def solution(mesh):
    return build(mesh, 400)
```

```python
import functools

import jax
import jax.numpy as jnp
from jax import lax
from jax.experimental import pallas as pl
from jax.experimental.pallas import tpu as pltpu
from jax.sharding import PartitionSpec as P

MESH = pl.DeviceIdType.MESH
SUBS = 4
TILES = 16
FLOOR = float(jnp.finfo(jnp.float32).min)
LINK_ORDER = ("H0", "W0", "W1", "H1", "W2", "H2", "F0", "F1", "W3", "H3", "W4", "F2", "F3", "W5", "W6", "W7")
H_TIME, W_TIME, STEP_TIME, EARLY_TIME, LAG = 33.9, 417.0, 2.4, 8.7, 3.0
CORE_LAG = 8.0
MAX_RUN = 2


def tile_of(q):
    if q < 4:
        return 0, q
    if q < 12:
        return 1 + q % 2, (q - 4) // 2
    return 3, q - 12


def link_order(n_chunks):
    tokens = [(t[0], int(t[1:])) for t in LINK_ORDER]
    last = max(k for kind, k in tokens if kind == "W")
    tokens = [t for t in tokens if t[0] != "W" or t[1] < n_chunks] + [("W", j) for j in range(last + 1, n_chunks)]
    start, after = [], [[], [], [], []]
    current = start
    for kind, k in tokens:
        if kind == "F":
            current = after[k // 2 * 2 + 1]
        current.append((kind, k))
    return start, after


def stretches(values):
    out, i = [], 0
    while i < len(values):
        n = 1
        while n < MAX_RUN and i + n < len(values) and values[i + n] == values[i] + n:
            n += 1
        out.append((n, values[i]))
        i += n
    return out


def plan(sizes):
    start, after = link_order(len(sizes))
    free, done, at = {"x": 0.0, "y": 0.0, "z": 0.0}, {}, {}
    tiles, chunks, cells, runs, pending, new = [], [], set(), [], [], []
    n_main = len(sizes) - 1

    def put(link, token, now):
        free[link] = max(free[link], now) + (W_TIME * sizes[token[1]] / sum(sizes) if token[0] == "W" else H_TIME)
        done[link, token] = free[link]

    def put_x(q, now):
        put("x", ("X", q), now)
        at["x", q] = free["x"] + LAG

    def issue(token, now):
        kind, k = token
        for link in "yz" if kind != "F" else "yz"[k % 2]:
            put(link, token, now)
        if kind == "F":
            at["diag", k] = done["yz"[k % 2], token] + LAG
        else:
            at["yz" if kind == "H" else "w", k] = max(done["y", token], done["z", token]) + LAG

    def handle(e, now):
        kind, k = e
        del at[e]
        pending.append(e)
        if kind == "x":
            at["h", k] = now + CORE_LAG
        elif kind == "h":
            new.append(k)
        elif kind == "yz":
            put_x(4 + 2 * k, now)
            put_x(5 + 2 * k, now)
            for token in after[k]:
                issue(token, now)
        elif kind == "diag":
            put_x(12 + k, now)
        elif k < n_main:
            chunks.append(k)

    def first():
        return min(at, key=lambda e: (at[e], e))

    for token in start:
        issue(token, 0.0)
    for q in range(4):
        put_x(q, 0.0)
    now = 0.0
    last_step = 0.0
    while len(cells) < TILES * n_main:
        while at and at[first()] <= now and len(new) < 2:
            handle(first(), now)
        options = [
            (n if n == 1 else n + 1.5, (0, q, 0, j, 1, n)) for q in sorted(tiles)
            for n, j in stretches([j for j in sorted(chunks) if (q, j) not in cells])]
        options += [
            (n, (0, q, 1, j, 0, n)) for j in sorted(chunks)
            for n, q in stretches([q for q in sorted(tiles) if (q, j) not in cells])]
        if new:
            run = (1, new.pop(0), 0, 0, 0, 1)
            tiles.append(run[1])
            now += last_step
            last_step = EARLY_TIME
        elif options:
            _, run = max(options, key=lambda o: o[0])
            _, q, dq, j, dj, n = run
            cells.update((q + dq * i, j + dj * i) for i in range(n))
            now += last_step + (n - 1) * STEP_TIME
            last_step = STEP_TIME
        else:
            e = first()
            now = max(now, at[e])
            handle(e, now)
            continue
        runs.append((pending[:], run))
        pending.clear()
    now += last_step
    while at:
        handle(first(), now)
    return runs, pending, now


def kernel(
    v_tile, h_ref, w_ref, ids_ref, q_ref, lp_ref, acc_ref, hbuf, early,
    wv, hv, he, staged, pin, lg, lg_end, ids_all, mx, sm, pk, st_send, st_recv,
    ss, rs, wss, wrs, wls, iss, irs, ils, sss, srs, lsem, hsem, esem, psem,
):
    rows, kp = h_ref.shape
    tile = rows // SUBS
    vocab = w_ref.shape[0]
    share = vocab // 4
    n_chunks = -(-share // v_tile)
    sizes = [min(v_tile, share - j * v_tile) for j in range(n_chunks)]
    runs, leftover, _ = plan(sizes)
    send_first, send_after = link_order(n_chunks)

    d, m = lax.axis_index("data"), lax.axis_index("model")
    y, z = lax.rem(d, 2), d // 2
    core, x = lax.rem(m, 2), m // 2
    m_sib = m + 1 - 2 * core
    m_x = m + 2 - 4 * x
    m_xs = m_sib + 2 - 4 * x

    def block(rb):
        ry, rz = rb % 2, rb // 2
        yy = 1 - y if ry else y
        zz = 1 - z if rz else z
        return zz * 2 + yy

    def row0(q):
        rb, sub = tile_of(q)
        return pl.multiple_of(block(rb) * rows + sub * tile, tile)

    def own_piece(q):
        rb, sub = tile_of(q)
        return h_ref.at[pl.ds(sub * tile, tile), :] if rb == 0 else hbuf.at[m, pl.ds(row0(q), tile), :]

    def send_h(src, q_here, q_there, mm, dev, sem):
        return pltpu.make_async_remote_copy(
            src_ref=src, dst_ref=hbuf.at[mm, pl.ds(row0(q_here), tile), :], send_sem=ss.at[sem],
            recv_sem=rs.at[q_there * 4 + mm], device_id=dev, device_id_type=MESH)

    def wait_h(q, mm):
        pltpu.make_async_remote_copy(
            src_ref=hbuf.at[mm, pl.ds(row0(q), tile), :], dst_ref=hbuf.at[mm, pl.ds(row0(q), tile), :],
            send_sem=ss.at[0], recv_sem=rs.at[q * 4 + mm], device_id=(d, m), device_id_type=MESH).wait_recv()

    def send_w(j, rb):
        size, dd = sizes[j], block(rb)
        return pltpu.make_async_remote_copy(
            src_ref=w_ref.at[pl.ds(pl.multiple_of(dd * share + j * v_tile, 8), size), :],
            dst_ref=wv.at[pl.ds(j * v_tile, size), pl.ds(rb * kp, kp)],
            send_sem=wss.at[j * 4 + rb], recv_sem=wrs.at[j * 4 + rb], device_id=(dd, m), device_id_type=MESH)

    def wait_w(j, rb):
        size = sizes[j]
        pltpu.make_async_remote_copy(
            src_ref=w_ref.at[pl.ds(0, size), :],
            dst_ref=wv.at[pl.ds(j * v_tile, size), pl.ds(rb * kp, kp)],
            send_sem=wss.at[j * 4 + rb], recv_sem=wrs.at[j * 4 + rb], device_id=(d, m), device_id_type=MESH).wait_recv()

    def local_w(j):
        size = sizes[j]
        return pltpu.make_async_copy(
            w_ref.at[pl.ds(pl.multiple_of(d * share + j * v_tile, 8), size), :],
            wv.at[pl.ds(j * v_tile, size), pl.ds(0, kp)], wls.at[j])

    def send_ids(rb):
        return pltpu.make_async_remote_copy(
            src_ref=ids_ref, dst_ref=ids_all.at[rb], send_sem=iss.at[rb], recv_sem=irs.at[rb],
            device_id=(block(rb), m), device_id_type=MESH)

    def put(kind, k):
        if kind == "H":
            send_h(own_piece(k), k, 4 + 2 * k, m, (block(1), m), 48 + k).start()
            send_h(own_piece(k), k, 5 + 2 * k, m, (block(2), m), 52 + k).start()
        elif kind == "F":
            q = 5 + 2 * k if k % 2 == 0 else 4 + 2 * k
            send_h(own_piece(q), q, 12 + k, m, (block(1 + k % 2), m), 56 + k).start()
        else:
            for rb in (3, 1, 2):
                send_w(k, rb).start()

    def spread(q):
        send_h(own_piece(q), q, q, m, (d, m_x), q).start()
        send_h(own_piece(q), q, q, m, (d, m_sib), 16 + q).start()

    def event(kind, k):
        if kind == "x":
            wait_h(k, m_x)
            send_h(hbuf.at[m_x, pl.ds(row0(k), tile), :], k, k, m_x, (d, m_sib), 32 + k).start()
        elif kind == "h":
            wait_h(k, m_sib)
            wait_h(k, m_xs)
            load_piece(jnp.int32(k), 0, he.at[k % 2], hsem.at[k % 2])
        elif kind == "yz":
            wait_h(4 + 2 * k, m)
            wait_h(5 + 2 * k, m)
            spread(4 + 2 * k)
            spread(5 + 2 * k)
            for token in send_after[k]:
                put(*token)
        elif kind == "diag":
            wait_h(12 + k, m)
            spread(12 + k)
        else:
            for rb in (1, 2, 3):
                wait_w(k, rb)

    def rb_sub(q):
        mid = q >= 4
        late = q >= 12
        rb = jnp.where(late, 3, jnp.where(mid, 1 + lax.rem(q, 2), 0))
        sub = jnp.where(late, q - 12, jnp.where(mid, (q - 4) // 2, q))
        return rb, sub

    def load_piece(q, part, dst, sem):
        rb, sub = rb_sub(q)
        ry, rz = lax.rem(rb, 2), rb // 2
        yy, zz = y + ry - 2 * y * ry, z + rz - 2 * z * rz
        row = pl.multiple_of((zz * 2 + yy) * rows + sub * tile, tile)
        mm = block(part)
        mine = jnp.logical_and(rb == 0, mm == m)

        @pl.when(mine)
        def _():
            pltpu.make_async_copy(h_ref.at[pl.ds(pl.multiple_of(sub * tile, tile), tile), :], dst, sem).start()

        @pl.when(jnp.logical_not(mine))
        def _():
            pltpu.make_async_copy(hbuf.at[mm, pl.ds(row, tile), :], dst, sem).start()

    def load_parts(q, slot):
        for part in (1, 2, 3):
            load_piece(q, part, hv.at[slot, :, pl.ds((part - 1) * kp, kp)], lsem.at[slot * 4 + part])

    def wait_parts(slot):
        for part in (1, 2, 3):
            pltpu.make_async_copy(
                h_ref.at[pl.ds(0, tile), :], hv.at[slot, :, pl.ds((part - 1) * kp, kp)], lsem.at[slot * 4 + part]).wait()

    def early_out(q, start, size, slot):
        return pltpu.make_async_copy(staged.at[slot, pl.ds(0, size), :], early.at[q, pl.ds(start, size), :], esem.at[slot])

    def early_in(q, start, size, slot):
        return pltpu.make_async_copy(early.at[q, pl.ds(start, size), :], pin.at[slot, pl.ds(0, size), :], psem.at[slot])

    own_ids = pltpu.make_async_copy(ids_ref, ids_all.at[0], ils)
    own_ids.start()
    for rb in (1, 2, 3):
        send_ids(rb).start()
    for i, token in enumerate(send_first):
        put(*token)
        if i == 0:
            for q in range(4):
                spread(q)
    for j in range(n_chunks):
        local_w(j).start()
    mx[...] = jnp.full(mx.shape, FLOOR, jnp.float32)
    sm[...] = jnp.zeros(sm.shape, jnp.float32)
    pk[...] = jnp.zeros(pk.shape, jnp.float32)
    lg[...] = jnp.full(lg.shape, -jnp.inf, jnp.float32)
    lg_end[...] = jnp.full(lg_end.shape, -jnp.inf, jnp.float32)
    own_ids.wait()
    for rb in (1, 2, 3):
        send_ids(rb).wait()
    for j in range(n_chunks):
        local_w(j).wait()

    base = m * vocab + d * share
    nowhere = jnp.int32(1 << 30)

    def dot(a, b):
        return lax.dot_general(a, b, (((1,), (1,)), ((), ())), preferred_element_type=jnp.float32)

    def product(start, size, slot, pslot):
        return dot(wv[pl.ds(start, size), kp:], hv[slot]) + pin[pslot, :size]

    end_start, end_size = (n_chunks - 1) * v_tile, sizes[-1]

    def early_products(q):
        half = lax.rem(q, 2)
        pltpu.make_async_copy(h_ref.at[pl.ds(0, tile), :], he.at[half], hsem.at[half]).wait()

        def one(j, carry):
            slot = lax.rem(j, 2)
            start = pl.multiple_of(j * v_tile, 8)
            pl.when(j >= 2)(lambda: early_out(q, start, v_tile, slot).wait())
            staged[slot] = dot(wv[pl.ds(start, v_tile), :kp], he[half])
            early_out(q, start, v_tile, slot).start()
            return carry

        lax.fori_loop(0, n_chunks - 1, one, 0)
        slot = (n_chunks - 1) % 2
        early_out(q, 0, v_tile, slot).wait()
        staged[slot, :end_size] = dot(wv[end_start:end_start + end_size, :kp], he[half])
        early_out(q, end_start, end_size, slot).start()
        early_out(q, 0, v_tile, 1 - slot).wait()
        early_out(q, end_start, end_size, slot).wait()

    def absorb(ref, q, start):
        rb, sub = rb_sub(q)
        size = ref.shape[0]
        spot = ids_all[rb, sub] - (base + start) - lax.broadcasted_iota(jnp.int32, (8, tile), 0)
        old = mx[q]
        new = old
        for k in range(0, size, 8):
            new = jnp.maximum(new, ref[k:k + 8, :])
        grown, picked = sm[q] * jnp.exp(old - new), pk[q]
        for k in range(0, size, 8):
            part = ref[k:k + 8, :]
            grown = grown + jnp.exp(part - new)
            picked = picked + jnp.where(spot == k, part, 0.0)
        mx[q] = new
        sm[q] = grown
        pk[q] = picked

    n_runs = len(runs)
    held, codes = TILES - 1, []
    for i, (_, (kind, q0, dq, j0, dj, n)) in enumerate(runs):
        following = runs[i + 1][1] if i + 1 < n_runs else (2, TILES - 1, 0, 0, 0, 1)
        held = q0 + dq * (n - 1) if kind == 0 else held
        q_next = held if following[0] == 1 else following[1]
        held = q_next
        code = 0
        for digit, radix in (
            (kind, 2), (q0, 16), (dq, 2), (j0, 8), (dj, 2), (n, 8), (q_next, 16), (following[3], 8), (following[0] == 0, 2)):
            code = code * radix + int(digit)
        codes.append(code)

    for e in runs[0][0]:
        event(*e)

    def run_body(r, carry):
        code = jnp.int32(codes[0])
        for i in range(1, n_runs):
            code = jnp.where(r >= i, jnp.int32(codes[i]), code)
        digits = []
        for radix in (2, 8, 16, 8, 2, 8, 2, 16, 2):
            digits.append(lax.rem(code, radix))
            code = code // radix
        next_main, j_next, q_next, n, dj, j0, dq, q0, kind = digits

        def step(i, carry):
            slot, slot_1, slot_2, fresh, held, pslot, q_old, start_old = carry
            q, j = q0 + dq * i, j0 + dj * i
            last = i == n - 1

            @pl.when(last)
            def _():
                for k in range(1, n_runs):
                    if runs[k][0]:
                        @pl.when(r == k - 1)
                        def _(k=k):
                            for e in runs[k][0]:
                                event(*e)

            q_new, j_new = jnp.where(last, q_next, q + dq), jnp.where(last, j_next, j + dj)
            more = jnp.where(last, next_main, 1) == 1
            after = pl.multiple_of(j_new * v_tile, 8)
            start = pl.multiple_of(j * v_tile, 8)
            load = q_new != held
            pl.when(load)(lambda: load_parts(q_new, slot_1))

            @pl.when(kind == 1)
            def _():
                early_products(q)
                pl.when(more)(lambda: early_in(q_new, after, v_tile, pslot).start())

            @pl.when(kind == 0)
            def _():
                pl.when(more)(lambda: early_in(q_new, after, v_tile, 1 - pslot).start())
                pl.when(fresh == 1)(lambda: wait_parts(slot))
                early_in(q, start, v_tile, pslot).wait()
                absorb(lg, q_old, start_old)
                lg[...] = product(start, v_tile, slot, pslot)

            main = kind == 0
            return (
                jnp.where(load, slot_1, slot), jnp.where(load, slot_2, slot_1), jnp.where(load, slot, slot_2),
                jnp.where(load, 1, jnp.where(main, 0, fresh)), q_new,
                jnp.where(main, 1 - pslot, pslot), jnp.where(main, q, q_old), jnp.where(main, start, start_old))

        return lax.fori_loop(0, n, step, carry)

    zero = jnp.int32(0)
    one, two = jnp.int32(1), jnp.int32(2)
    slot, slot_1, slot_2, fresh, _, pslot, q_old, start_old = lax.fori_loop(
        0, n_runs, run_body, (zero, one, two, zero, jnp.int32(TILES - 1), zero, zero, nowhere))

    lanes = 128
    me = d * 4 + m

    def finish(rb):
        for q in [q for q in range(TILES) if tile_of(q)[0] == rb]:
            sub = tile_of(q)[1]
            old = mx[q]
            top = jnp.max(old, axis=0, keepdims=True)
            parts = (
                top, jnp.sum(sm[q] * jnp.exp(old - top), axis=0, keepdims=True), jnp.sum(pk[q], axis=0, keepdims=True))
            for k, part in enumerate(parts):
                for i in range(tile // lanes):
                    st_send[rb, k, pl.ds(sub * (tile // lanes) + i, 1), :] = part[:, i * lanes:(i + 1) * lanes]

    def send_stats(rb, o):
        return pltpu.make_async_remote_copy(
            src_ref=st_send.at[rb], dst_ref=st_recv.at[me], send_sem=sss.at[rb * 4 + o], recv_sem=srs.at[me],
            device_id=(block(rb), lax.rem(m + o, 4)), device_id_type=MESH)

    others = [(rb, o) for rb in (3, 2, 1, 0) for o in range(4) if (rb, o) != (0, 0)]

    def send_blocks(*blocks):
        for rb, o in others:
            if rb in blocks:
                send_stats(rb, o).start()

    load_parts(jnp.int32(TILES - 2), slot_1)
    early_in(TILES - 1, end_start, end_size, pslot).start()
    absorb(lg, q_old, start_old)
    for e in leftover:
        event(*e)

    def end_step(i, carry):
        slot, slot_1, slot_2, fresh, pslot, q_old, start_old = carry
        q = TILES - 1 - i
        pl.when(q > 1)(lambda: load_parts(q - 2, slot_2))

        @pl.when(q > 0)
        def _():
            early_in(q - 1, end_start, end_size, 1 - pslot).start()

        pl.when(q == 10)(lambda: finish(3))
        pl.when(q == 9)(lambda: send_blocks(3))
        pl.when(q == 2)(lambda: [finish(1), finish(2)] and None)
        pl.when(q == 1)(lambda: send_blocks(2, 1))
        pl.when(fresh == 1)(lambda: wait_parts(slot))
        early_in(q, end_start, end_size, pslot).wait()
        absorb(lg_end, q_old, start_old)
        lg_end[...] = product(end_start, end_size, slot, pslot)
        return slot_1, slot_2, slot, jnp.int32(1), 1 - pslot, q, jnp.int32(end_start)

    *_, q_old, start_old = lax.fori_loop(
        0, TILES, end_step, (slot, slot_1, slot_2, fresh, pslot, jnp.int32(TILES - 1), nowhere))
    absorb(lg_end, q_old, start_old)
    finish(0)

    def drain(i, carry):
        pltpu.make_async_remote_copy(
            src_ref=h_ref.at[pl.ds(0, tile), :], dst_ref=hbuf.at[0, pl.ds(0, tile), :], send_sem=ss.at[i],
            recv_sem=rs.at[0], device_id=(d, m), device_id_type=MESH).wait_send()
        return carry

    lax.fori_loop(0, 60, drain, 0)
    for j in range(n_chunks):
        for rb in (1, 2, 3):
            send_w(j, rb).wait_send()
    st_recv[me] = st_send[0]
    send_blocks(0)
    for rb, o in others:
        send_stats(rb, o).wait_send()
    for rb, o in others:
        source = block(rb) * 4 + lax.rem(m + o, 4)
        pltpu.make_async_remote_copy(
            src_ref=st_send.at[rb], dst_ref=st_recv.at[source], send_sem=sss.at[rb * 4 + o], recv_sem=srs.at[source],
            device_id=(d, m), device_id_type=MESH).wait_recv()

    top = jnp.max(st_recv[:, 0], axis=0)
    total = jnp.sum(st_recv[:, 1] * jnp.exp(st_recv[:, 0] - top[None]), axis=0)
    picked = jnp.sum(st_recv[:, 2], axis=0)
    log_prob = picked - (top + jnp.log(total))
    lp_ref[...] = log_prob
    acc_ref[...] = jnp.minimum(1.0, jnp.exp(log_prob) / q_ref[...])


def build(mesh, v_tile):
    def per_device(h_part, w_part, draft_loc, q_loc):
        rows, kp = h_part.shape
        vocab = w_part.shape[0]
        share, tile = vocab // 4, rows // SUBS
        n_chunks = -(-share // v_tile)
        lanes = 128
        flat = (rows // lanes, lanes)
        dma, vmem = pltpu.SemaphoreType.DMA, pltpu.VMEM
        any_space = pl.BlockSpec(memory_space=pl.ANY)
        in_vmem = pl.BlockSpec(memory_space=pltpu.VMEM)
        lp, acc, _, _ = pl.pallas_call(
            functools.partial(kernel, v_tile),
            out_shape=(
                jax.ShapeDtypeStruct(flat, jnp.float32),
                jax.ShapeDtypeStruct(flat, jnp.float32),
                jax.ShapeDtypeStruct((4, 4 * rows, kp), jnp.bfloat16),
                jax.ShapeDtypeStruct((TILES, share, tile), jnp.float32),
            ),
            in_specs=[any_space, any_space, in_vmem, in_vmem],
            out_specs=(in_vmem, in_vmem, any_space, any_space),
            scratch_shapes=[
                vmem((share, 4 * kp), jnp.bfloat16),
                vmem((3, tile, 3 * kp), jnp.bfloat16),
                vmem((2, tile, kp), jnp.bfloat16),
                vmem((2, v_tile, tile), jnp.float32),
                vmem((2, v_tile, tile), jnp.float32),
                vmem((v_tile, tile), jnp.float32),
                vmem((share - (n_chunks - 1) * v_tile, tile), jnp.float32),
                vmem((4, SUBS, 1, tile), jnp.int32),
                vmem((TILES, 8, tile), jnp.float32),
                vmem((TILES, 8, tile), jnp.float32),
                vmem((TILES, 8, tile), jnp.float32),
                vmem((4, 3) + flat, jnp.float32),
                vmem((16, 3) + flat, jnp.float32),
                dma((60,)), dma((64,)), dma((4 * n_chunks,)), dma((4 * n_chunks,)), dma((n_chunks,)),
                dma((4,)), dma((4,)), dma, dma((16,)), dma((16,)), dma((12,)), dma((2,)), dma((2,)), dma((2,)),
            ],
            compiler_params=pltpu.CompilerParams(has_side_effects=True, vmem_limit_bytes=67_043_328),
            name="head",
        )(h_part, w_part, draft_loc.reshape(SUBS, 1, tile), q_loc.reshape(flat))
        return lp.reshape(rows), acc.reshape(rows)

    return jax.shard_map(
        per_device, mesh=mesh, in_specs=(P("data", "model"), P("model", "data"), P("data"), P("data")),
        out_specs=(P("data"), P("data")), check_vma=False)


def solution(mesh):
    return build(mesh, 400)
```
